32 devices in a mesh: rep: 2 (over y), dev: 4 (over z), col: 4 (over x, core).
Axes of the slice: x: 2, y: 2, z: 4, core: 2. Of those that a mesh axis runs over, the one named last changes fastest.
Arguments:
- queries: bfloat16 [256, 8192], P(('rep', 'dev'), 'col'), parts along dimension 0
- kv_pages: bfloat16 [768, 8, 2, 128, 128], P(('rep', 'dev'), 'col'), parts along dimension 0
- page_table: int32 [256, 3], P(('rep', 'dev')), parts along dimension 0, may hold values from 0 to 95, as said below
- seq_lengths: int32 [256], P(('rep', 'dev')), parts along dimension 0, may hold values from 2 to 384, as said below
- ffn_seat: int32 [256], P('rep'), parts along dimension 0, may hold values from 0 to 127, each once
- resid: bfloat16 [256, 8192], P(('rep', 'col'), 'dev'), parts along dimension 0, may hold values from -6 to 6
- w_out: bfloat16 [8192, 8192], P('col', 'dev'), may hold values from -0.0625 to 0.0625
- norm_gain: float32 [8192], P('dev'), may hold values from 0.25 to 1.75
- w_gate: bfloat16 [8192, 14336], P('dev', 'col'), may hold values from -0.0625 to 0.0625
- w_up: bfloat16 [8192, 14336], P('dev', 'col'), may hold values from -0.0625 to 0.0625
- w_down: bfloat16 [14336, 8192], P('col', 'dev'), may hold values from -0.046875 to 0.046875
Outputs:
- layer_out: bfloat16 [256, 8192], P(('rep', 'col'), 'dev'), parts along dimension 0
The draws below stay inside these ranges and needn't reach their ends.
There are 2 independent parts, one for each index of `rep`. The reference program is written for one: setup_inputs(seed, part) draws one part's arguments, and reference() takes and returns one part's arrays. A program takes and returns all parts, laid end to end along the dimension named above; an argument that names none is the same for every part. Nothing has to cross between parts.
Inputs may be any that keep to these rules, and one draw needn't show every extreme that they name: `page_table`: the 32 rows of one dev index hold each block 0 to 95 of that index's pool exactly once. `seq_lengths`: the first sequence has 384 cached tokens.
All inputs are finite; a program needn't handle non-finite values.
Results may differ from the reference program's by a relative error of at most 0.017.
Values may be sent and summed in bfloat16 or wider, within the bound.
A program may use at most 128 MiB of HBM per device.

```python
import jax
import jax.numpy as jnp
from jax import lax

HQ = 64
KVH = 8
HD = 128
D = 8192
FF = 14336
SEQ_DEV = 32
PAGE = 128
MAXP = 3
POOL = 96
MAXLEN = 384
TOKENS = 128
N_DEV = 4


def layout_ints(key):
    base = jax.random.fold_in(key, 101)
    first_key, second_key, third_key = jax.random.split(base, 3)
    ceilings = jax.random.randint(first_key, (N_DEV, 1), MAXLEN // 4, MAXLEN + 1)
    raw_bits = jax.random.randint(second_key, (N_DEV, SEQ_DEV), 0, 1 << 30)
    lengths = 2 + raw_bits % (ceilings - 1)
    lengths = lengths.reshape(-1).at[0].set(MAXLEN)
    group_keys = jax.random.split(third_key, N_DEV)
    tables = jax.vmap(lambda one_key: jax.random.permutation(one_key, POOL))(group_keys)
    return (lengths.astype(jnp.int32), tables.reshape(SEQ_DEV * N_DEV, MAXP).astype(jnp.int32))


def draw_seq_lengths(key, part):
    return layout_ints(key)[0]


def draw_page_table(key, part):
    return layout_ints(key)[1]


def draw_kv_pages(key, part):
    values = jnp.clip(jax.random.normal(jax.random.fold_in(key, 202), (N_DEV * POOL, KVH, 2, PAGE, HD), jnp.float32), -5.0, 5.0)
    return values.astype(jnp.bfloat16)


def draw_queries(key, part):
    tokens = SEQ_DEV * N_DEV
    query = jnp.clip(jax.random.normal(jax.random.fold_in(key, 301), (tokens, HQ, HD), jnp.float32), -5.0, 5.0)
    return query.reshape(tokens, HQ * HD).astype(jnp.bfloat16)


def block_levels(key, dims, cuts, smallest, largest):
    level, own = 1.0, jax.random.fold_in(key, 6)
    for position, blocks in cuts:
        steps = jnp.exp(jax.random.uniform(jax.random.fold_in(own, position), (blocks,), jnp.float32, smallest / len(cuts), largest / len(cuts)))
        level = level * jnp.repeat(steps, dims[position] // blocks).reshape([-1 if axis == position else 1 for axis in range(len(dims))])
    return level


def scatter_about(stream_key, extent, spread, bound, cuts=(), kind=jnp.bfloat16):
    array = spread * jax.random.normal(stream_key, extent, jnp.float32)
    if cuts:
        array = array * block_levels(stream_key, extent, cuts, -0.22, 0.18)
    return jnp.clip(array, -bound, bound).astype(kind)


def setup_inputs(seed: int = 0, part: int = 0) -> dict:
    seeds = jax.random.split(jax.random.key(seed), 12)
    part_splits = jax.random.split(jax.random.fold_in(seeds[11], part), 12)
    return {
        "queries": draw_queries(jax.random.fold_in(jax.random.fold_in(seeds[11], part), 71), part),
        "kv_pages": draw_kv_pages(jax.random.fold_in(jax.random.fold_in(seeds[11], part), 71), part),
        "page_table": draw_page_table(jax.random.fold_in(jax.random.fold_in(seeds[11], part), 71), part),
        "seq_lengths": draw_seq_lengths(jax.random.fold_in(jax.random.fold_in(seeds[11], part), 71), part),
        "ffn_seat": jax.random.permutation(part_splits[4], TOKENS).astype(jnp.int32),
        "resid": scatter_about(part_splits[5], (TOKENS, D), 1.0, 6.0, ((0, 4), (1, 4))),
        "w_out": scatter_about(seeds[6], (D, D), D ** -0.5, 0.0625, ((0, 4), (1, 4))),
        "norm_gain": jnp.clip(1.0 + 0.15 * jax.random.normal(seeds[7], (D,), jnp.float32), 0.25, 1.75),
        "w_gate": scatter_about(seeds[8], (D, FF), D ** -0.5, 0.0625, ((0, 4), (1, 4))),
        "w_up": scatter_about(seeds[9], (D, FF), D ** -0.5, 0.0625, ((0, 4), (1, 4))),
        "w_down": scatter_about(seeds[10], (FF, D), FF ** -0.5, 0.046875, ((0, 4), (1, 4))),
    }


def attend_group(operands):
    query, kv_group, table, lengths = operands
    group_size = HQ // KVH
    kv_blocks = kv_group[table]
    key_span = MAXP * PAGE
    key_rows = kv_blocks[:, :, :, 0].transpose(0, 2, 1, 3, 4).reshape(SEQ_DEV, KVH, key_span, HD)
    value_rows = kv_blocks[:, :, :, 1].transpose(0, 2, 1, 3, 4).reshape(SEQ_DEV, KVH, key_span, HD)
    query_heads = query.reshape(SEQ_DEV, KVH, group_size, HD)
    scores = jnp.einsum('skgd,sktd->skgt', query_heads.astype(jnp.float32), key_rows.astype(jnp.float32)) * HD ** (-0.5)
    live_mask = jnp.arange(key_span)[None, :] < lengths[:, None]
    scores = jnp.where(live_mask[:, None, None, :], scores, -1e+30)
    top = lax.optimization_barrier(jnp.max(scores, axis=-1, keepdims=True))
    expo = jnp.exp(scores - top)
    weights = (expo / lax.optimization_barrier(jnp.sum(expo, axis=-1, keepdims=True))).astype(jnp.bfloat16)
    attended = jnp.einsum('skgt,sktd->skgd', weights.astype(jnp.float32), value_rows.astype(jnp.float32))
    return attended.astype(jnp.bfloat16).reshape(SEQ_DEV, HQ * HD)

def reference(queries, kv_pages, page_table, seq_lengths, ffn_seat, resid, w_out, norm_gain, w_gate, w_up, w_down):
    width = HQ * HD
    attended = lax.map(attend_group, (queries.reshape(N_DEV, SEQ_DEV, width), kv_pages.reshape(N_DEV, POOL, KVH, 2, PAGE, HD), page_table.reshape(N_DEV, SEQ_DEV, MAXP), seq_lengths.reshape(N_DEV, SEQ_DEV)))
    attended = attended.reshape(SEQ_DEV * N_DEV, width)
    projected = jnp.dot(attended, w_out, preferred_element_type=jnp.float32)
    placed = jnp.zeros_like(projected).at[ffn_seat].set(projected)
    stream = resid.astype(jnp.float32) + placed
    mean_sq = lax.optimization_barrier(jnp.mean(stream * stream, axis=1))
    normed = (stream * lax.rsqrt(mean_sq + 1e-05)[:, None] * norm_gain[None, :]).astype(jnp.bfloat16)
    gate = jnp.dot(normed, w_gate, preferred_element_type=jnp.float32)
    up_part = jnp.dot(normed, w_up, preferred_element_type=jnp.float32)
    hidden = (jax.nn.silu(gate) * up_part).astype(jnp.bfloat16)
    ffn_out = jnp.dot(hidden, w_down, preferred_element_type=jnp.float32)
    return (stream + ffn_out).astype(jnp.bfloat16)
```

```python
import functools

import jax
import jax.numpy as jnp
from jax import lax
from jax.experimental import pallas as pl
from jax.experimental.pallas import tpu as pltpu
from jax.sharding import PartitionSpec as P

MESH = pl.DeviceIdType.MESH
F32 = jnp.float32
BF16 = jnp.bfloat16
TILE = 128
SUB = 8


def divisor(size, choices):
    for choice in choices:
        if size % choice == 0:
            return choice
    return size


def layer_kernel(
    nd,
    nc,
    dims,
    table_hbm,
    len_hbm,
    q_hbm,
    kv_hbm,
    seat_hbm,
    resid_hbm,
    gain_hbm,
    wo_hbm,
    wg_hbm,
    wu_hbm,
    wd_hbm,
    out_hbm,
    table,
    lens,
    q_in,
    seat,
    resid,
    gain,
    wo,
    wg,
    wu,
    kpool,
    vpool,
    q_rows,
    o_rows,
    scores,
    att_all,
    seated,
    proj,
    rs_one,
    rs_mid,
    rs_two,
    x_all,
    stream,
    own,
    in_r,
    in_l,
    ss_own,
    ss_r,
    ss_l,
    inv,
    hid,
    acc,
    down,
    dn_one,
    dn_mid,
    dn_two,
    out,
    in_sem,
    kv_sem,
    w_sem,
    att_s,
    att_r,
    one_s,
    one_r,
    two_s,
    two_r,
    x_s,
    x_r,
    pair_s,
    pair_r,
    sum_s,
    sum_r,
    ssd_s,
    ssd_r,
    hid_s,
    hid_r,
    done_s,
    done_r,
    dtwo_s,
    dtwo_r,
):
    T, B, R, HK, DK, FK, kvl, group, pages, blocks, WC, NJ, CF, NC, half, NX, full = dims
    me = lax.axis_index("dev")
    mc = lax.axis_index("col")
    mx, core = mc // 2, mc % 2
    E = nd - 1
    heads = kvl * group
    span = pages * TILE
    KB = DK // TILE
    FB = FK // TILE
    KH = (KB + 1) // 2
    partner = {"col": mx * 2 + 1 - core}

    def x_peer(k):
        return lax.rem(mx + k, NX)

    def x_from(k):
        return lax.rem(mx + NX - k, NX)

    small = [
        pltpu.make_async_copy(table_hbm, table, in_sem.at[0]),
        pltpu.make_async_copy(len_hbm, lens, in_sem.at[1]),
        pltpu.make_async_copy(q_hbm, q_in, in_sem.at[2]),
        pltpu.make_async_copy(seat_hbm, seat, in_sem.at[3]),
        pltpu.make_async_copy(resid_hbm, resid, in_sem.at[4]),
        pltpu.make_async_copy(gain_hbm, gain, in_sem.at[5]),
    ]
    kv_count = blocks * kvl
    kv_copies = [
        pltpu.make_async_copy(
            kv_hbm.at[:, v], (kpool, vpool)[v].at[pl.ds(0, kv_count)], kv_sem.at[v]
        )
        for v in (0, 1)
    ]
    w_copies = [
        pltpu.make_async_copy(wo_hbm, wo, w_sem.at[0]),
        pltpu.make_async_copy(wg_hbm, wg, w_sem.at[1]),
        pltpu.make_async_copy(wu_hbm, wu, w_sem.at[2]),
    ]

    def wd_copy(n):
        cols = slice(n * TILE, (n + 1) * TILE)
        return pltpu.make_async_copy(
            wd_hbm.at[:, :, cols],
            (kpool, vpool)[n // KH].at[pl.ds(n % KH * FB, FB)],
            w_sem.at[3 + n],
        )

    for copy in small[:3]:
        copy.start()
    for copy in kv_copies:
        copy.start()
    for copy in small[3:]:
        copy.start()

    barrier = pltpu.get_barrier_semaphore()

    @pl.when(me > 0)
    def _():
        pl.semaphore_signal(barrier, inc=1, device_id={"dev": me - 1}, device_id_type=MESH)

    @pl.when(me < E)
    def _():
        pl.semaphore_signal(barrier, inc=1, device_id={"dev": me + 1}, device_id_type=MESH)

    for k in range(1, NX):
        pl.semaphore_signal(
            barrier, inc=1, device_id={"col": x_peer(k) * 2 + core}, device_id_type=MESH
        )
    pl.semaphore_signal(barrier, inc=1, device_id=partner, device_id_type=MESH)

    small[2].wait()
    for n in range(heads):
        q_rows[pl.ds(n, B, stride=heads), :] = q_in[:, n * TILE : (n + 1) * TILE].astype(F32)
    small[0].wait()
    small[1].wait()
    kv_copies[0].wait()
    w_copies[0].start()

    neighbours = jnp.where(me > 0, 1, 0) + jnp.where(me < E, 1, 0)

    PB = B // 2
    scale = TILE ** (-0.5)
    head_row = lax.broadcasted_iota(jnp.int32, (heads, TILE), 0) // group

    def blocked(value):
        if kvl == 1:
            return value.astype(BF16)
        wide = lax.broadcasted_iota(jnp.int32, value.shape, 0) // group
        return jnp.concatenate(
            [jnp.where(wide == h, value, 0.0).astype(BF16) for h in range(kvl)], axis=1
        )

    def att_copy(origin, a, way):
        spot = att_all.at[pl.ds(pl.multiple_of(origin * B + a * PB, PB), PB), :]
        return pltpu.make_async_remote_copy(
            src_ref=spot,
            dst_ref=spot,
            send_sem=att_s.at[way, origin, a],
            recv_sem=att_r.at[origin, a],
            device_id={"dev": me + (1 if way == 0 else -1)},
            device_id_type=MESH,
        )

    for a in range(2):
        @pl.loop(0, PB // SUB)
        def _(b):
            for u in range(SUB):
                spot = b * SUB + u
                s = a * PB + spot
                rows = pl.ds(pl.multiple_of(s * heads, heads), heads)
                query = blocked(q_rows[rows, :])
                keys = []
                for j in range(pages):
                    block = table[j, s]
                    keys.append(
                        jnp.concatenate([kpool[block * kvl + h] for h in range(kvl)], axis=1)
                        if kvl > 1
                        else kpool[block]
                    )
                value = lax.dot_general(
                    query,
                    jnp.concatenate(keys, axis=0),
                    (((1,), (1,)), ((), ())),
                    preferred_element_type=F32,
                ) * scale
                live = lax.broadcasted_iota(jnp.int32, value.shape, 1) < lens[s]
                scores[pl.ds(pl.multiple_of(spot * heads, heads), heads), :] = jnp.where(
                    live, value, -1e30
                )

        if a == 0:
            kv_copies[1].wait()
            w_copies[1].start()
            w_copies[2].start()

        @pl.loop(0, PB // SUB)
        def _(b):
            rows = pl.ds(pl.multiple_of(b * (SUB * heads), SUB * heads), SUB * heads)
            value = scores[rows, :]
            expo = jnp.exp(value - jnp.max(value, axis=1, keepdims=True))
            scores[rows, :] = expo / jnp.sum(expo, axis=1, keepdims=True)
            for u in range(SUB):
                spot = b * SUB + u
                s = a * PB + spot
                weights = blocked(
                    scores[pl.ds(pl.multiple_of(spot * heads, heads), heads), :]
                )
                vals = [
                    vpool[table[j, s] * kvl + h]
                    for h in range(kvl)
                    for j in range(pages)
                ]
                o_rows[pl.ds(pl.multiple_of(spot * heads, heads), heads), :] = jnp.dot(
                    weights, jnp.concatenate(vals, axis=0), preferred_element_type=F32
                )

        mine = pl.ds(pl.multiple_of(me * B + a * PB, PB), PB)
        for n in range(heads):
            att_all[mine, n * TILE : (n + 1) * TILE] = o_rows[
                pl.ds(n, PB, stride=heads), :
            ].astype(BF16)

        if a == 0:
            pl.semaphore_wait(barrier, neighbours + NX)

        @pl.when(me < E)
        def _():
            att_copy(me, a, 0).start()

        @pl.when(me > 0)
        def _():
            att_copy(me, a, 1).start()

    for n in range(KB):
        wd_copy(n).start()

    for copy in small[3:]:
        copy.wait()

    @pl.loop(1, nd)
    def _(k):
        for a in range(2):
            @pl.when(me - k >= 0)
            def _():
                att_copy(me - k, a, 0).wait_recv()

                @pl.when(me < E)
                def _():
                    att_copy(me - k, a, 0).start()

            @pl.when(me + k <= E)
            def _():
                att_copy(me + k, a, 1).wait_recv()

                @pl.when(me > 0)
                def _():
                    att_copy(me + k, a, 1).start()

    place = lax.broadcasted_iota(jnp.int32, (T, T), 0)
    position = place // R
    seat_here = ((position % NX) * 2 + position // NX) * R + place % R
    pick = (seat_here == seat[...]).astype(F32).astype(BF16)
    seated[...] = jnp.dot(pick, att_all[...], preferred_element_type=F32).astype(BF16)

    half_rows = NX * R
    my_half = pl.ds(pl.multiple_of(core * half_rows, half_rows), half_rows)
    other_half = pl.ds(pl.multiple_of((1 - core) * half_rows, half_rows), half_rows)

    def block_rows(c, x):
        return pl.ds(pl.multiple_of((c * NX + x) * R, R), R)

    my_rows = block_rows(core, mx)
    mid_own = pl.ds(pl.multiple_of(mx * R, R), R)

    def one_copy(j, source, target, send, recv):
        cols = slice(j * WC, (j + 1) * WC)
        return pltpu.make_async_remote_copy(
            src_ref=source.at[other_half, cols],
            dst_ref=target.at[:, cols],
            send_sem=send.at[j],
            recv_sem=recv.at[j],
            device_id=partner,
            device_id_type=MESH,
        )

    def two_copy(k, j, source, target, send, recv):
        cols = slice(j * WC, (j + 1) * WC)
        rows = pl.ds(pl.multiple_of(x_peer(k) * R, R), R)
        return pltpu.make_async_remote_copy(
            src_ref=source.at[rows, cols],
            dst_ref=target.at[k - 1, :, cols],
            send_sem=send.at[k - 1, j],
            recv_sem=recv.at[k - 1, j],
            device_id={"col": x_peer(k) * 2 + core},
            device_id_type=MESH,
        )

    one_args = (proj, rs_one, one_s, one_r)
    two_args = (rs_mid, rs_two, two_s, two_r)
    done_args = (down, dn_one, done_s, done_r)
    dtwo_args = (dn_mid, dn_two, dtwo_s, dtwo_r)

    def meet(j, source, arrived, middle, one, two):
        cols = slice(j * WC, (j + 1) * WC)
        one_copy(j, *one).wait_recv()
        middle[:, cols] = (
            source[my_half, cols].astype(F32) + arrived[:, cols].astype(F32)
        ).astype(BF16)
        for k in range(1, NX):
            two_copy(k, j, *two).start()

    w_copies[0].wait()
    for j in range(NJ + 1):
        if j < NJ:
            cols = slice(j * WC, (j + 1) * WC)
            proj[:, cols] = jnp.dot(
                seated[...], wo[:, cols], preferred_element_type=F32
            ).astype(BF16)
            one_copy(j, *one_args).start()
        if j > 0:
            meet(j - 1, proj, rs_one, rs_mid, one_args, two_args)

    def x_copy(k, j):
        spot = x_all.at[my_rows, j * WC : (j + 1) * WC]
        return pltpu.make_async_remote_copy(
            src_ref=spot,
            dst_ref=spot,
            send_sem=x_s.at[k - 1, j],
            recv_sem=x_r.at[k - 1, j],
            device_id={"col": x_peer(k) * 2 + core},
            device_id_type=MESH,
        )

    def pair_copy(k, j):
        spot = x_all.at[block_rows(core, x_from(k)), j * WC : (j + 1) * WC]
        return pltpu.make_async_remote_copy(
            src_ref=spot,
            dst_ref=spot,
            send_sem=pair_s.at[k, j],
            recv_sem=pair_r.at[k, j],
            device_id=partner,
            device_id_type=MESH,
        )

    for j in range(NJ):
        cols = slice(j * WC, (j + 1) * WC)
        value = (
            resid[:, cols].astype(F32)
            + proj[my_rows, cols].astype(F32)
            + rs_one[mid_own, cols].astype(F32)
        )
        for k in range(1, NX):
            two_copy(k, j, *two_args).wait_recv()
            value = value + rs_two[k - 1, :, cols].astype(F32)
        stream[:, cols] = value
        x_all[my_rows, cols] = (value * gain[:, cols]).astype(BF16)
        for k in range(1, NX):
            x_copy(k, j).start()
        pair_copy(0, j).start()
    for j in range(NJ):
        for k in range(1, NX):
            x_copy(k, j).wait_recv()
            pair_copy(k, j).start()
    for j in range(NJ):
        for k in range(NX):
            pair_copy(k, j).wait_recv()

    def neighbour(way):
        return {"dev": me + (1 if way == 0 else -1)}

    def sum_copy(way, c):
        return pltpu.make_async_remote_copy(
            src_ref=own.at[c, 1 - way],
            dst_ref=(in_r if way == 0 else in_l).at[c],
            send_sem=sum_s.at[way, c],
            recv_sem=sum_r.at[way, c],
            device_id=neighbour(way),
            device_id_type=MESH,
        )

    def ssd_copy(way):
        return pltpu.make_async_remote_copy(
            src_ref=ss_own.at[pl.ds((1 - way) * half, half), :],
            dst_ref=ss_r if way == 0 else ss_l,
            send_sem=ssd_s.at[way],
            recv_sem=ssd_r.at[way],
            device_id=neighbour(way),
            device_id_type=MESH,
        )

    def hid_copy(way, c):
        spot = hid.at[c, pl.ds(way * half, half), :]
        return pltpu.make_async_remote_copy(
            src_ref=spot,
            dst_ref=spot,
            send_sem=hid_s.at[way, c],
            recv_sem=hid_r.at[way, c],
            device_id=neighbour(way),
            device_id_type=MESH,
        )

    def sum_stage(way, c):
        first = 0 if way == 0 else E
        last = E - first
        part = 1 - way
        incoming = in_r if way == 0 else in_l
        ss_in = ss_r if way == 0 else ss_l
        ss_rows = pl.ds(part * half, half)

        @pl.when(c == 0)
        def _():
            ssd_copy(way).wait_recv()
            ss_own[ss_rows, :] = ss_own[ss_rows, :] + ss_in[...]

            @pl.when(me != last)
            def _():
                ssd_copy(way).start()

            @pl.when(me == last)
            def _():
                inv[...] = lax.rsqrt(ss_own[ss_rows, :] / full + 1e-5)

        sum_copy(way, c).wait_recv()

        @pl.when(me != last)
        def _():
            total = own[c, part].astype(F32) + incoming[c].astype(F32)
            own[c, part] = total.astype(BF16)
            sum_copy(way, c).start()

        @pl.when(me == last)
        def _():
            total = own[c, part].astype(F32) + incoming[c].astype(F32)
            factor = inv[:, 0:1]
            gate = total[:, :CF] * factor
            up = total[:, CF:] * factor
            hid[c, part * half : (part + 1) * half, :] = (
                gate / (1.0 + jnp.exp(-gate)) * up
            ).astype(BF16)
            hid_copy(part, c).start()

    def hid_stage(way, c):
        last = E if way == 0 else 0
        hid_copy(way, c).wait_recv()

        @pl.when(me != last)
        def _():
            hid_copy(way, c).start()

    def inside(c):
        return jnp.logical_and(c >= 0, c < NC)

    PACE = 2

    def sum_lag(d):
        return (5 * d + 1) // 2

    first_hid = max(NC + 2, (5 * E + 1) // 2 + 1)

    def hid_lag(d):
        return first_hid + (5 * (d - 1)) // 2

    acc[...] = jnp.zeros_like(acc)
    w_copies[1].wait()
    w_copies[2].wait()

    @pl.loop(0, NC + first_hid + (5 * (E - 1)) // 2)
    def _(i):
        for p in range(PACE):
            q = i * PACE + p

            @pl.when(q < NC)
            def _():
                cols = pl.ds(pl.multiple_of(q * CF, CF), CF)
                gate = jnp.dot(x_all[...], wg[:, cols], preferred_element_type=F32).astype(BF16)
                own[q, 0, :, :CF] = gate[:half]
                own[q, 1, :, :CF] = gate[half:]
                up = jnp.dot(x_all[...], wu[:, cols], preferred_element_type=F32).astype(BF16)
                own[q, 0, :, CF:] = up[:half]
                own[q, 1, :, CF:] = up[half:]
                for way in (0, 1):
                    @pl.when(me == (0 if way == 0 else E))
                    def _():
                        sum_copy(way, q).start()

        @pl.when(i == 0)
        def _():
            squares = jnp.zeros((T, 1), F32)
            for j in range(NJ):
                cols = slice(j * WC, (j + 1) * WC)
                value = x_all[:, cols].astype(F32) / gain[:, cols]
                squares = squares + jnp.sum(value * value, axis=1, keepdims=True)
            ss_own[...] = jnp.broadcast_to(squares, (T, ss_own.shape[1]))
            for way in (0, 1):
                @pl.when(me == (0 if way == 0 else E))
                def _():
                    ssd_copy(way).start()

        for way in (0, 1):
            d = me if way == 0 else E - me
            c = i - sum_lag(d)

            @pl.when(jnp.logical_and(d > 0, inside(c)))
            def _():
                sum_stage(way, c)

        for way in (0, 1):
            d = me if way == 0 else E - me
            c = i - hid_lag(d)

            @pl.when(jnp.logical_and(d > 0, inside(c)))
            def _():
                hid_stage(way, c)

        c = i - hid_lag(jnp.maximum(me, E - me))

        @pl.when(i == hid_lag(jnp.maximum(me, E - me)))
        def _():
            for n in range(KB):
                wd_copy(n).wait()

        @pl.when(inside(c))
        def _():
            per = CF // TILE
            wide = 2 if KB % 2 == 0 else 1
            value = hid[c]
            for n in range(0, KB, wide):
                right = [
                    (kpool, vpool)[(n + w) // KH][
                        pl.ds((n + w) % KH * FB + c * per, per)
                    ].reshape(CF, TILE)
                    for w in range(wide)
                ]
                cols = slice(n * TILE, (n + wide) * TILE)
                acc[:, cols] += jnp.dot(
                    value, jnp.concatenate(right, axis=1), preferred_element_type=F32
                )

    for j in range(NJ + 1):
        if j < NJ:
            cols = slice(j * WC, (j + 1) * WC)
            down[:, cols] = acc[:, cols].astype(BF16)
            one_copy(j, *done_args).start()
        if j > 0:
            meet(j - 1, down, dn_one, dn_mid, done_args, dtwo_args)
    for j in range(NJ):
        cols = slice(j * WC, (j + 1) * WC)
        value = stream[:, cols] + acc[my_rows, cols] + dn_one[mid_own, cols].astype(F32)
        for k in range(1, NX):
            two_copy(k, j, *dtwo_args).wait_recv()
            value = value + dn_two[k - 1, :, cols].astype(F32)
        out[:, cols] = value.astype(BF16)
    result = pltpu.make_async_copy(out, out_hbm, in_sem.at[0])
    result.start()

    for j in range(NJ):
        one_copy(j, *one_args).wait_send()
        one_copy(j, *done_args).wait_send()
        for k in range(1, NX):
            two_copy(k, j, *two_args).wait_send()
            two_copy(k, j, *dtwo_args).wait_send()
            x_copy(k, j).wait_send()
        for k in range(NX):
            pair_copy(k, j).wait_send()

    for a in range(2):
        @pl.loop(0, nd)
        def _(origin):
            @pl.when(jnp.logical_and(me < E, origin <= me))
            def _():
                att_copy(origin, a, 0).wait_send()

            @pl.when(jnp.logical_and(me > 0, origin >= me))
            def _():
                att_copy(origin, a, 1).wait_send()

    for way in (0, 1):
        @pl.when(me != (E if way == 0 else 0))
        def _():
            ssd_copy(way).wait_send()

            @pl.loop(0, NC)
            def _(c):
                sum_copy(way, c).wait_send()
                hid_copy(way, c).wait_send()
    result.wait()


def solution(mesh):
    nd, nc = mesh.shape["dev"], mesh.shape["col"]

    def on_device(
        queries,
        kv_pages,
        page_table,
        seq_lengths,
        ffn_seat,
        resid,
        w_out,
        norm_gain,
        w_gate,
        w_up,
        w_down,
    ):
        B, HK = queries.shape
        blocks, kvl, _, page, head_dim = kv_pages.shape
        pages = page_table.shape[1]
        group = HK // (kvl * head_dim)
        heads = kvl * group
        T = ffn_seat.shape[0]
        R, DK = resid.shape
        FK = w_gate.shape[1]
        WC = divisor(DK, (512, 256, 128))
        NJ = DK // WC
        CF = divisor(FK, (256, 128))
        NC = FK // CF
        half = T // 2
        NX = nc // 2
        KB, FB = DK // TILE, FK // TILE
        dims = (
            T, B, R, HK, DK, FK, kvl, group, pages, blocks, WC, NJ, CF, NC, half, NX, float(DK * nd)
        )
        dma = pltpu.SemaphoreType.DMA
        hbm = pl.BlockSpec(memory_space=pltpu.HBM)
        vmem = pltpu.VMEM
        PB = B // 2
        scratch = [
            pltpu.SMEM((pages, B), jnp.int32),
            pltpu.SMEM((B,), jnp.int32),
            vmem((B, HK), BF16),
            vmem((1, T), jnp.int32),
            vmem((R, DK), BF16),
            vmem((1, DK), F32),
            vmem((HK, DK), BF16),
            vmem((DK, FK), BF16),
            vmem((DK, FK), BF16),
            vmem((max(blocks * kvl, (KB + 1) // 2 * FB), TILE, TILE), BF16),
            vmem((max(blocks * kvl, (KB + 1) // 2 * FB), TILE, TILE), BF16),
            vmem((B * heads, head_dim), F32),
            vmem((PB * heads, head_dim), F32),
            vmem((PB * heads, pages * page), F32),
            vmem((T, HK), BF16),
            vmem((T, HK), BF16),
            vmem((T, DK), BF16),
            vmem((NX * R, DK), BF16),
            vmem((NX * R, DK), BF16),
            vmem((max(NX - 1, 1), R, DK), BF16),
            vmem((T, DK), BF16),
            vmem((R, DK), F32),
            vmem((NC, 2, half, 2 * CF), BF16),
            vmem((NC, half, 2 * CF), BF16),
            vmem((NC, half, 2 * CF), BF16),
            vmem((T, 128), F32),
            vmem((half, 128), F32),
            vmem((half, 128), F32),
            vmem((half, 128), F32),
            vmem((NC, T, CF), BF16),
            vmem((T, DK), F32),
            vmem((T, DK), BF16),
            vmem((NX * R, DK), BF16),
            vmem((NX * R, DK), BF16),
            vmem((max(NX - 1, 1), R, DK), BF16),
            vmem((R, DK), BF16),
            dma((6,)),
            dma((2,)),
            dma((3 + KB,)),
            dma((2, nd, 2)),
            dma((nd, 2)),
            dma((NJ,)),
            dma((NJ,)),
            dma((max(NX - 1, 1), NJ)),
            dma((max(NX - 1, 1), NJ)),
            dma((max(NX - 1, 1), NJ)),
            dma((max(NX - 1, 1), NJ)),
            dma((NX, NJ)),
            dma((NX, NJ)),
            dma((2, NC)),
            dma((2, NC)),
            dma((2,)),
            dma((2,)),
            dma((2, NC)),
            dma((2, NC)),
            dma((NJ,)),
            dma((NJ,)),
            dma((max(NX - 1, 1), NJ)),
            dma((max(NX - 1, 1), NJ)),
        ]
        return pl.pallas_call(
            functools.partial(layer_kernel, nd, nc, dims),
            out_shape=jax.ShapeDtypeStruct((R, DK), BF16),
            in_specs=[hbm] * 11,
            out_specs=hbm,
            scratch_shapes=scratch,
            compiler_params=pltpu.CompilerParams(
                collective_id=0, has_side_effects=True, vmem_limit_bytes=67043328
            ),
        )(
            page_table.T,
            seq_lengths,
            queries,
            kv_pages.reshape(blocks * kvl, 2, page, head_dim),
            ffn_seat[None, :],
            resid,
            norm_gain[None, :],
            w_out,
            w_gate,
            w_up,
            w_down.reshape(FB, TILE, DK),
        )

    in_specs = (
        P(("rep", "dev"), "col"),
        P(("rep", "dev"), "col", None, None, None),
        P(("rep", "dev"), None),
        P(("rep", "dev")),
        P("rep"),
        P(("rep", "col"), "dev"),
        P("col", "dev"),
        P("dev"),
        P("dev", "col"),
        P("dev", "col"),
        P("col", "dev"),
    )
    return jax.shard_map(
        on_device,
        mesh=mesh,
        in_specs=in_specs,
        out_specs=P(("rep", "col"), "dev"),
        check_vma=False,
    )
```

```python
import functools

import jax
import jax.numpy as jnp
from jax import lax
from jax.experimental import pallas as pl
from jax.experimental.pallas import tpu as pltpu
from jax.sharding import PartitionSpec as P

MESH = pl.DeviceIdType.MESH
F32 = jnp.float32
BF16 = jnp.bfloat16
TILE = 128
SUB = 8
LAG_S0, LAG_S, LAG_H0, LAG_H = 4, 3, 4, 5


def divisor(size, choices):
    for choice in choices:
        if size % choice == 0:
            return choice
    return size


def layer_kernel(
    nd,
    nc,
    dims,
    table_hbm,
    len_hbm,
    q_hbm,
    kv_hbm,
    seat_hbm,
    resid_hbm,
    gain_hbm,
    wo_hbm,
    wg_hbm,
    wu_hbm,
    wd_hbm,
    out_hbm,
    table,
    lens,
    q_in,
    seat,
    resid,
    gain,
    wo,
    wg,
    wu,
    kpool,
    vpool,
    q_rows,
    o_rows,
    scores,
    att_all,
    seated,
    proj,
    rs_one,
    rs_mid,
    rs_two,
    x_all,
    stream,
    own,
    in_r,
    in_l,
    ss_own,
    ss_r,
    ss_l,
    inv,
    hid,
    acc,
    down,
    dn_one,
    dn_mid,
    dn_two,
    out,
    in_sem,
    kv_sem,
    w_sem,
    att_s,
    att_r,
    one_s,
    one_r,
    two_s,
    two_r,
    x_s,
    x_r,
    pair_s,
    pair_r,
    sum_s,
    sum_r,
    ssd_s,
    ssd_r,
    hid_s,
    hid_r,
    done_s,
    done_r,
    dtwo_s,
    dtwo_r,
):
    T, B, R, HK, DK, FK, kvl, group, pages, blocks, WC, NJ, CF, NC, half, NX, full = dims
    me = lax.axis_index("dev")
    mc = lax.axis_index("col")
    mx, core = mc // 2, mc % 2
    E = nd - 1
    heads = kvl * group
    span = pages * TILE
    KB = DK // TILE
    FB = FK // TILE
    KH = (KB + 1) // 2
    partner = {"col": mx * 2 + 1 - core}

    def x_peer(k):
        return lax.rem(mx + k, NX)

    def x_from(k):
        return lax.rem(mx + NX - k, NX)

    small = [
        pltpu.make_async_copy(table_hbm, table, in_sem.at[0]),
        pltpu.make_async_copy(len_hbm, lens, in_sem.at[1]),
        pltpu.make_async_copy(q_hbm, q_in, in_sem.at[2]),
        pltpu.make_async_copy(seat_hbm, seat, in_sem.at[3]),
        pltpu.make_async_copy(resid_hbm, resid, in_sem.at[4]),
        pltpu.make_async_copy(gain_hbm, gain, in_sem.at[5]),
    ]
    kv_count = blocks * kvl
    kv_copies = [
        pltpu.make_async_copy(
            kv_hbm.at[:, v], (kpool, vpool)[v].at[pl.ds(0, kv_count)], kv_sem.at[v]
        )
        for v in (0, 1)
    ]
    w_copies = [
        pltpu.make_async_copy(wo_hbm, wo, w_sem.at[0]),
        pltpu.make_async_copy(wg_hbm, wg, w_sem.at[1]),
        pltpu.make_async_copy(wu_hbm, wu, w_sem.at[2]),
    ]

    def wd_copy(n):
        cols = slice(n * TILE, (n + 1) * TILE)
        return pltpu.make_async_copy(
            wd_hbm.at[:, :, cols],
            (kpool, vpool)[n // KH].at[pl.ds(n % KH * FB, FB)],
            w_sem.at[3 + n],
        )

    for copy in small[:3]:
        copy.start()
    for copy in kv_copies:
        copy.start()
    for copy in small[3:]:
        copy.start()

    barrier = pltpu.get_barrier_semaphore()

    @pl.when(me > 0)
    def _():
        pl.semaphore_signal(barrier, inc=1, device_id={"dev": me - 1}, device_id_type=MESH)

    @pl.when(me < E)
    def _():
        pl.semaphore_signal(barrier, inc=1, device_id={"dev": me + 1}, device_id_type=MESH)

    for k in range(1, NX):
        pl.semaphore_signal(
            barrier, inc=1, device_id={"col": x_peer(k) * 2 + core}, device_id_type=MESH
        )
    pl.semaphore_signal(barrier, inc=1, device_id=partner, device_id_type=MESH)

    small[2].wait()
    for n in range(heads):
        q_rows[pl.ds(n, B, stride=heads), :] = q_in[:, n * TILE : (n + 1) * TILE].astype(F32)
    small[0].wait()
    small[1].wait()
    kv_copies[0].wait()
    w_copies[0].start()

    neighbours = jnp.where(me > 0, 1, 0) + jnp.where(me < E, 1, 0)
    PB = B // 2
    scale = TILE ** (-0.5)
    head_row = lax.broadcasted_iota(jnp.int32, (heads, TILE), 0) // group

    def blocked(value):
        if kvl == 1:
            return value.astype(BF16)
        wide = lax.broadcasted_iota(jnp.int32, value.shape, 0) // group
        return jnp.concatenate(
            [jnp.where(wide == h, value, 0.0).astype(BF16) for h in range(kvl)], axis=1
        )

    def att_copy(origin, a, way):
        spot = att_all.at[pl.ds(pl.multiple_of(origin * B + a * PB, PB), PB), :]
        return pltpu.make_async_remote_copy(
            src_ref=spot,
            dst_ref=spot,
            send_sem=att_s.at[way, origin, a],
            recv_sem=att_r.at[origin, a],
            device_id={"dev": me + (1 if way == 0 else -1)},
            device_id_type=MESH,
        )

    for a in range(2):
        @pl.loop(0, PB // SUB)
        def _(b):
            for u in range(SUB):
                spot = b * SUB + u
                s = a * PB + spot
                rows = pl.ds(pl.multiple_of(s * heads, heads), heads)
                query = blocked(q_rows[rows, :])
                keys = []
                for j in range(pages):
                    block = table[j, s]
                    keys.append(
                        jnp.concatenate([kpool[block * kvl + h] for h in range(kvl)], axis=1)
                        if kvl > 1
                        else kpool[block]
                    )
                value = lax.dot_general(
                    query,
                    jnp.concatenate(keys, axis=0),
                    (((1,), (1,)), ((), ())),
                    preferred_element_type=F32,
                ) * scale
                live = lax.broadcasted_iota(jnp.int32, value.shape, 1) < lens[s]
                scores[pl.ds(pl.multiple_of(spot * heads, heads), heads), :] = jnp.where(
                    live, value, -1e30
                )

        if a == 0:
            kv_copies[1].wait()
            w_copies[1].start()
            w_copies[2].start()

        @pl.loop(0, PB // SUB)
        def _(b):
            rows = pl.ds(pl.multiple_of(b * (SUB * heads), SUB * heads), SUB * heads)
            value = scores[rows, :]
            expo = jnp.exp(value - jnp.max(value, axis=1, keepdims=True))
            scores[rows, :] = expo / jnp.sum(expo, axis=1, keepdims=True)
            for u in range(SUB):
                spot = b * SUB + u
                s = a * PB + spot
                weights = blocked(
                    scores[pl.ds(pl.multiple_of(spot * heads, heads), heads), :]
                )
                vals = [
                    vpool[table[j, s] * kvl + h]
                    for h in range(kvl)
                    for j in range(pages)
                ]
                o_rows[pl.ds(pl.multiple_of(spot * heads, heads), heads), :] = jnp.dot(
                    weights, jnp.concatenate(vals, axis=0), preferred_element_type=F32
                )

        mine = pl.ds(pl.multiple_of(me * B + a * PB, PB), PB)
        for n in range(heads):
            att_all[mine, n * TILE : (n + 1) * TILE] = o_rows[
                pl.ds(n, PB, stride=heads), :
            ].astype(BF16)

        if a == 0:
            pl.semaphore_wait(barrier, neighbours + NX)

        @pl.when(me < E)
        def _():
            att_copy(me, a, 0).start()

        @pl.when(me > 0)
        def _():
            att_copy(me, a, 1).start()

    for n in range(KB):
        wd_copy(n).start()

    for copy in small[3:]:
        copy.wait()

    @pl.loop(1, nd)
    def _(k):
        for a in range(2):
            @pl.when(me - k >= 0)
            def _():
                att_copy(me - k, a, 0).wait_recv()

                @pl.when(me < E)
                def _():
                    att_copy(me - k, a, 0).start()

            @pl.when(me + k <= E)
            def _():
                att_copy(me + k, a, 1).wait_recv()

                @pl.when(me > 0)
                def _():
                    att_copy(me + k, a, 1).start()

    place = lax.broadcasted_iota(jnp.int32, (T, T), 0)
    position = place // R
    seat_here = ((position % NX) * 2 + position // NX) * R + place % R
    pick = (seat_here == seat[...]).astype(F32).astype(BF16)
    seated[...] = jnp.dot(pick, att_all[...], preferred_element_type=F32).astype(BF16)

    half_rows = NX * R
    my_half = pl.ds(pl.multiple_of(core * half_rows, half_rows), half_rows)
    other_half = pl.ds(pl.multiple_of((1 - core) * half_rows, half_rows), half_rows)

    def block_rows(c, x):
        return pl.ds(pl.multiple_of((c * NX + x) * R, R), R)

    my_rows = block_rows(core, mx)
    mid_own = pl.ds(pl.multiple_of(mx * R, R), R)

    def one_copy(j, source, target, send, recv):
        cols = slice(j * WC, (j + 1) * WC)
        return pltpu.make_async_remote_copy(
            src_ref=source.at[other_half, cols],
            dst_ref=target.at[:, cols],
            send_sem=send.at[j],
            recv_sem=recv.at[j],
            device_id=partner,
            device_id_type=MESH,
        )

    def two_copy(k, j, source, target, send, recv):
        cols = slice(j * WC, (j + 1) * WC)
        rows = pl.ds(pl.multiple_of(x_peer(k) * R, R), R)
        return pltpu.make_async_remote_copy(
            src_ref=source.at[rows, cols],
            dst_ref=target.at[k - 1, :, cols],
            send_sem=send.at[k - 1, j],
            recv_sem=recv.at[k - 1, j],
            device_id={"col": x_peer(k) * 2 + core},
            device_id_type=MESH,
        )

    one_args = (proj, rs_one, one_s, one_r)
    two_args = (rs_mid, rs_two, two_s, two_r)
    done_args = (down, dn_one, done_s, done_r)
    dtwo_args = (dn_mid, dn_two, dtwo_s, dtwo_r)

    def meet(j, source, arrived, middle, one, two):
        cols = slice(j * WC, (j + 1) * WC)
        one_copy(j, *one).wait_recv()
        middle[:, cols] = (
            source[my_half, cols].astype(F32) + arrived[:, cols].astype(F32)
        ).astype(BF16)
        for k in range(1, NX):
            two_copy(k, j, *two).start()

    w_copies[0].wait()
    for j in range(NJ + 1):
        if j < NJ:
            cols = slice(j * WC, (j + 1) * WC)
            proj[:, cols] = jnp.dot(
                seated[...], wo[:, cols], preferred_element_type=F32
            ).astype(BF16)
            one_copy(j, *one_args).start()
        if j > 0:
            meet(j - 1, proj, rs_one, rs_mid, one_args, two_args)

    def x_copy(k, j):
        spot = x_all.at[my_rows, j * WC : (j + 1) * WC]
        return pltpu.make_async_remote_copy(
            src_ref=spot,
            dst_ref=spot,
            send_sem=x_s.at[k - 1, j],
            recv_sem=x_r.at[k - 1, j],
            device_id={"col": x_peer(k) * 2 + core},
            device_id_type=MESH,
        )

    def pair_copy(k, j):
        spot = x_all.at[block_rows(core, x_from(k)), j * WC : (j + 1) * WC]
        return pltpu.make_async_remote_copy(
            src_ref=spot,
            dst_ref=spot,
            send_sem=pair_s.at[k, j],
            recv_sem=pair_r.at[k, j],
            device_id=partner,
            device_id_type=MESH,
        )

    for j in range(NJ):
        cols = slice(j * WC, (j + 1) * WC)
        value = (
            resid[:, cols].astype(F32)
            + proj[my_rows, cols].astype(F32)
            + rs_one[mid_own, cols].astype(F32)
        )
        for k in range(1, NX):
            two_copy(k, j, *two_args).wait_recv()
            value = value + rs_two[k - 1, :, cols].astype(F32)
        stream[:, cols] = value
        x_all[my_rows, cols] = (value * gain[:, cols]).astype(BF16)
        for k in range(1, NX):
            x_copy(k, j).start()
        pair_copy(0, j).start()
    for j in range(NJ):
        for k in range(1, NX):
            x_copy(k, j).wait_recv()
            pair_copy(k, j).start()
    for j in range(NJ):
        for k in range(NX):
            pair_copy(k, j).wait_recv()

    def neighbour(way):
        return {"dev": me + (1 if way == 0 else -1)}

    def sum_copy(way, c):
        return pltpu.make_async_remote_copy(
            src_ref=own.at[c, 1 - way],
            dst_ref=(in_r if way == 0 else in_l).at[c],
            send_sem=sum_s.at[way, c],
            recv_sem=sum_r.at[way, c],
            device_id=neighbour(way),
            device_id_type=MESH,
        )

    def ssd_copy(way):
        return pltpu.make_async_remote_copy(
            src_ref=ss_own.at[pl.ds((1 - way) * half, half), :],
            dst_ref=ss_r if way == 0 else ss_l,
            send_sem=ssd_s.at[way],
            recv_sem=ssd_r.at[way],
            device_id=neighbour(way),
            device_id_type=MESH,
        )

    def hid_copy(way, c):
        spot = hid.at[c, pl.ds(way * half, half), :]
        return pltpu.make_async_remote_copy(
            src_ref=spot,
            dst_ref=spot,
            send_sem=hid_s.at[way, c],
            recv_sem=hid_r.at[way, c],
            device_id=neighbour(way),
            device_id_type=MESH,
        )

    def sum_stage(way, c):
        first = 0 if way == 0 else E
        last = E - first
        part = 1 - way
        incoming = in_r if way == 0 else in_l
        ss_in = ss_r if way == 0 else ss_l
        ss_rows = pl.ds(part * half, half)

        @pl.when(c == jnp.where(me == last, 0, min(1, NC - 1)))
        def _():
            ssd_copy(way).wait_recv()
            ss_own[ss_rows, :] = ss_own[ss_rows, :] + ss_in[...]

            @pl.when(me != last)
            def _():
                ssd_copy(way).start()

            @pl.when(me == last)
            def _():
                inv[...] = lax.rsqrt(ss_own[ss_rows, :] / full + 1e-5)

        sum_copy(way, c).wait_recv()

        @pl.when(me != last)
        def _():
            total = own[c, part].astype(F32) + incoming[c].astype(F32)
            own[c, part] = total.astype(BF16)
            sum_copy(way, c).start()

        @pl.when(me == last)
        def _():
            total = own[c, part].astype(F32) + incoming[c].astype(F32)
            factor = inv[:, 0:1]
            gate = total[:, :CF] * factor
            up = total[:, CF:] * factor
            hid[c, part * half : (part + 1) * half, :] = (
                gate / (1.0 + jnp.exp(-gate)) * up
            ).astype(BF16)
            hid_copy(part, c).start()

    def hid_stage(way, c):
        last = E if way == 0 else 0
        hid_copy(way, c).wait_recv()

        @pl.when(me != last)
        def _():
            hid_copy(way, c).start()

    def inside(c):
        return jnp.logical_and(c >= 0, c < NC)

    PACE = 2

    def sum_lag(d):
        return LAG_S0 + LAG_S * (d - 1)

    first_hid = max(NC + LAG_H0, sum_lag(E) + 1)

    def hid_lag(d):
        return first_hid + LAG_H * (d - 1)

    acc[...] = jnp.zeros_like(acc)
    w_copies[1].wait()
    w_copies[2].wait()

    @pl.loop(0, NC + hid_lag(E))
    def _(i):
        for p in range(PACE):
            q = i * PACE + p

            @pl.when(q < NC)
            def _():
                cols = pl.ds(pl.multiple_of(q * CF, CF), CF)
                gate = jnp.dot(x_all[...], wg[:, cols], preferred_element_type=F32).astype(BF16)
                own[q, 0, :, :CF] = gate[:half]
                own[q, 1, :, :CF] = gate[half:]
                up = jnp.dot(x_all[...], wu[:, cols], preferred_element_type=F32).astype(BF16)
                own[q, 0, :, CF:] = up[:half]
                own[q, 1, :, CF:] = up[half:]
                for way in (0, 1):
                    @pl.when(me == (0 if way == 0 else E))
                    def _():
                        sum_copy(way, q).start()

        @pl.when(i == 0)
        def _():
            squares = jnp.zeros((T, 1), F32)
            for j in range(NJ):
                cols = slice(j * WC, (j + 1) * WC)
                value = x_all[:, cols].astype(F32) / gain[:, cols]
                squares = squares + jnp.sum(value * value, axis=1, keepdims=True)
            ss_own[...] = jnp.broadcast_to(squares, (T, ss_own.shape[1]))
            for way in (0, 1):
                @pl.when(me == (0 if way == 0 else E))
                def _():
                    ssd_copy(way).start()

        for way in (0, 1):
            d = me if way == 0 else E - me
            c = i - sum_lag(d)

            @pl.when(jnp.logical_and(d > 0, inside(c)))
            def _():
                sum_stage(way, c)

        for way in (0, 1):
            d = me if way == 0 else E - me
            c = i - hid_lag(d)

            @pl.when(jnp.logical_and(d > 0, inside(c)))
            def _():
                hid_stage(way, c)

        c = i - hid_lag(jnp.maximum(me, E - me))

        @pl.when(i == hid_lag(jnp.maximum(me, E - me)))
        def _():
            for n in range(KB):
                wd_copy(n).wait()

        @pl.when(inside(c))
        def _():
            per = CF // TILE
            wide = 2 if KB % 2 == 0 else 1
            value = hid[c]
            for n in range(0, KB, wide):
                right = [
                    (kpool, vpool)[(n + w) // KH][
                        pl.ds((n + w) % KH * FB + c * per, per)
                    ].reshape(CF, TILE)
                    for w in range(wide)
                ]
                cols = slice(n * TILE, (n + wide) * TILE)
                acc[:, cols] += jnp.dot(
                    value, jnp.concatenate(right, axis=1), preferred_element_type=F32
                )

    for j in range(NJ + 1):
        if j < NJ:
            cols = slice(j * WC, (j + 1) * WC)
            down[:, cols] = acc[:, cols].astype(BF16)
            one_copy(j, *done_args).start()
        if j > 0:
            meet(j - 1, down, dn_one, dn_mid, done_args, dtwo_args)
    for j in range(NJ):
        cols = slice(j * WC, (j + 1) * WC)
        value = stream[:, cols] + acc[my_rows, cols] + dn_one[mid_own, cols].astype(F32)
        for k in range(1, NX):
            two_copy(k, j, *dtwo_args).wait_recv()
            value = value + dn_two[k - 1, :, cols].astype(F32)
        out[:, cols] = value.astype(BF16)
    result = pltpu.make_async_copy(out, out_hbm, in_sem.at[0])
    result.start()

    for j in range(NJ):
        one_copy(j, *one_args).wait_send()
        one_copy(j, *done_args).wait_send()
        for k in range(1, NX):
            two_copy(k, j, *two_args).wait_send()
            two_copy(k, j, *dtwo_args).wait_send()
            x_copy(k, j).wait_send()
        for k in range(NX):
            pair_copy(k, j).wait_send()

    for a in range(2):
        @pl.loop(0, nd)
        def _(origin):
            @pl.when(jnp.logical_and(me < E, origin <= me))
            def _():
                att_copy(origin, a, 0).wait_send()

            @pl.when(jnp.logical_and(me > 0, origin >= me))
            def _():
                att_copy(origin, a, 1).wait_send()

    for way in (0, 1):
        @pl.when(me != (E if way == 0 else 0))
        def _():
            ssd_copy(way).wait_send()

            @pl.loop(0, NC)
            def _(c):
                sum_copy(way, c).wait_send()
                hid_copy(way, c).wait_send()

    result.wait()


def solution(mesh):
    nd, nc = mesh.shape["dev"], mesh.shape["col"]

    def on_device(
        queries,
        kv_pages,
        page_table,
        seq_lengths,
        ffn_seat,
        resid,
        w_out,
        norm_gain,
        w_gate,
        w_up,
        w_down,
    ):
        B, HK = queries.shape
        blocks, kvl, _, page, head_dim = kv_pages.shape
        pages = page_table.shape[1]
        group = HK // (kvl * head_dim)
        heads = kvl * group
        T = ffn_seat.shape[0]
        R, DK = resid.shape
        FK = w_gate.shape[1]
        WC = divisor(DK, (512, 256, 128))
        NJ = DK // WC
        CF = divisor(FK, (256, 128))
        NC = FK // CF
        half = T // 2
        NX = nc // 2
        KB, FB = DK // TILE, FK // TILE
        dims = (
            T, B, R, HK, DK, FK, kvl, group, pages, blocks, WC, NJ, CF, NC, half, NX, float(DK * nd)
        )
        dma = pltpu.SemaphoreType.DMA
        hbm = pl.BlockSpec(memory_space=pltpu.HBM)
        vmem = pltpu.VMEM
        PB = B // 2
        scratch = [
            pltpu.SMEM((pages, B), jnp.int32),
            pltpu.SMEM((B,), jnp.int32),
            vmem((B, HK), BF16),
            vmem((1, T), jnp.int32),
            vmem((R, DK), BF16),
            vmem((1, DK), F32),
            vmem((HK, DK), BF16),
            vmem((DK, FK), BF16),
            vmem((DK, FK), BF16),
            vmem((max(blocks * kvl, (KB + 1) // 2 * FB), TILE, TILE), BF16),
            vmem((max(blocks * kvl, (KB + 1) // 2 * FB), TILE, TILE), BF16),
            vmem((B * heads, head_dim), F32),
            vmem((PB * heads, head_dim), F32),
            vmem((PB * heads, pages * page), F32),
            vmem((T, HK), BF16),
            vmem((T, HK), BF16),
            vmem((T, DK), BF16),
            vmem((NX * R, DK), BF16),
            vmem((NX * R, DK), BF16),
            vmem((max(NX - 1, 1), R, DK), BF16),
            vmem((T, DK), BF16),
            vmem((R, DK), F32),
            vmem((NC, 2, half, 2 * CF), BF16),
            vmem((NC, half, 2 * CF), BF16),
            vmem((NC, half, 2 * CF), BF16),
            vmem((T, 128), F32),
            vmem((half, 128), F32),
            vmem((half, 128), F32),
            vmem((half, 128), F32),
            vmem((NC, T, CF), BF16),
            vmem((T, DK), F32),
            vmem((T, DK), BF16),
            vmem((NX * R, DK), BF16),
            vmem((NX * R, DK), BF16),
            vmem((max(NX - 1, 1), R, DK), BF16),
            vmem((R, DK), BF16),
            dma((6,)),
            dma((2,)),
            dma((3 + KB,)),
            dma((2, nd, 2)),
            dma((nd, 2)),
            dma((NJ,)),
            dma((NJ,)),
            dma((max(NX - 1, 1), NJ)),
            dma((max(NX - 1, 1), NJ)),
            dma((max(NX - 1, 1), NJ)),
            dma((max(NX - 1, 1), NJ)),
            dma((NX, NJ)),
            dma((NX, NJ)),
            dma((2, NC)),
            dma((2, NC)),
            dma((2,)),
            dma((2,)),
            dma((2, NC)),
            dma((2, NC)),
            dma((NJ,)),
            dma((NJ,)),
            dma((max(NX - 1, 1), NJ)),
            dma((max(NX - 1, 1), NJ)),
        ]
        return pl.pallas_call(
            functools.partial(layer_kernel, nd, nc, dims),
            out_shape=jax.ShapeDtypeStruct((R, DK), BF16),
            in_specs=[hbm] * 11,
            out_specs=hbm,
            scratch_shapes=scratch,
            compiler_params=pltpu.CompilerParams(
                collective_id=0, has_side_effects=True, vmem_limit_bytes=67043328
            ),
        )(
            page_table.T,
            seq_lengths,
            queries,
            kv_pages.reshape(blocks * kvl, 2, page, head_dim),
            ffn_seat[None, :],
            resid,
            norm_gain[None, :],
            w_out,
            w_gate,
            w_up,
            w_down.reshape(FB, TILE, DK),
        )

    in_specs = (
        P(("rep", "dev"), "col"),
        P(("rep", "dev"), "col", None, None, None),
        P(("rep", "dev"), None),
        P(("rep", "dev")),
        P("rep"),
        P(("rep", "col"), "dev"),
        P("col", "dev"),
        P("dev"),
        P("dev", "col"),
        P("dev", "col"),
        P("col", "dev"),
    )
    return jax.shard_map(
        on_device,
        mesh=mesh,
        in_specs=in_specs,
        out_specs=P(("rep", "col"), "dev"),
        check_vma=False,
    )
```

```python
import functools

import jax
import jax.numpy as jnp
from jax import lax
from jax.experimental import pallas as pl
from jax.experimental.pallas import tpu as pltpu
from jax.sharding import PartitionSpec as P

MESH = pl.DeviceIdType.MESH
F32 = jnp.float32
BF16 = jnp.bfloat16
TILE = 128
SUB = 8
LATER = 3
PART = 2
WCM = 1024
LAG_S0 = 4
LAG_S = 3
LAG_H0 = 4
LAG_H = 5


def divisor(size, choices):
    for choice in choices:
        if size % choice == 0:
            return choice
    return size


def layer_kernel(
    nd,
    nc,
    dims,
    table_hbm,
    len_hbm,
    q_hbm,
    kv_hbm,
    seat_hbm,
    resid_hbm,
    gain_hbm,
    wo_hbm,
    wg_hbm,
    wu_hbm,
    wd_hbm,
    out,
    table,
    lens,
    q_in,
    seat,
    resid_all,
    resid_rows,
    pick,
    gain,
    wo,
    wg,
    wu,
    kpool,
    vpool,
    q_rows,
    o_rows,
    scores,
    att_all,
    proj,
    rs_one,
    rs_mid,
    rs_two,
    x_all,
    stream,
    own,
    in_r,
    in_l,
    ss_own,
    ss_r,
    ss_l,
    inv,
    hid,
    acc,
    down,
    dn_one,
    dn_mid,
    dn_two,
    in_sem,
    kv_sem,
    w_sem,
    att_s,
    att_r,
    res_s,
    res_r,
    one_s,
    one_r,
    two_s,
    two_r,
    x_s,
    x_r,
    pair_s,
    pair_r,
    sum_s,
    sum_r,
    ssd_s,
    ssd_r,
    hid_s,
    hid_r,
    done_s,
    done_r,
    dtwo_s,
    dtwo_r,
):
    T, B, R, HK, DK, FK, kvl, group, pages, blocks, WC, NJ, CF, NC, half, NX, full = dims
    RH = half // nc
    PACE = 2
    PHASE = (NC + PACE - 1) // PACE
    me = lax.axis_index("dev")
    mc = lax.axis_index("col")
    mx, core = mc // 2, mc % 2
    E = nd - 1
    late_dev = (me * 2) // nd
    halves = (late_dev, 1 - late_dev)
    heads = kvl * group
    span = pages * TILE
    KB = DK // TILE
    FB = FK // TILE
    KH = (KB + 1) // 2
    partner = {"col": mx * 2 + 1 - core}

    def peer_of(k):
        return lax.rem(mc + k, nc)

    def x_peer(k):
        return lax.rem(mx + k, NX)

    def x_from(k):
        return lax.rem(mx + NX - k, NX)

    small = [
        pltpu.make_async_copy(table_hbm, table, in_sem.at[0]),
        pltpu.make_async_copy(len_hbm, lens, in_sem.at[1]),
        pltpu.make_async_copy(q_hbm, q_in, in_sem.at[2]),
        pltpu.make_async_copy(seat_hbm, seat, in_sem.at[3]),
        pltpu.make_async_copy(
            resid_hbm, resid_all.at[pl.ds(pl.multiple_of(mc * R, R), R), :], in_sem.at[4]
        ),
        pltpu.make_async_copy(gain_hbm, gain, in_sem.at[5]),
    ]
    kv_count = blocks * kvl
    kv_copies = [
        pltpu.make_async_copy(
            kv_hbm.at[:, v], (kpool, vpool)[v].at[pl.ds(0, kv_count)], kv_sem.at[v]
        )
        for v in (0, 1)
    ]
    w_copies = [
        pltpu.make_async_copy(wo_hbm, wo, w_sem.at[0]),
        pltpu.make_async_copy(wg_hbm, wg, w_sem.at[1]),
        pltpu.make_async_copy(wu_hbm, wu, w_sem.at[2]),
    ]

    def wd_copy(n):
        cols = slice(n * TILE, (n + 1) * TILE)
        return pltpu.make_async_copy(
            wd_hbm.at[:, :, cols],
            (kpool, vpool)[n // KH].at[pl.ds(n % KH * FB, FB)],
            w_sem.at[3 + n // KH],
        )

    def wd_wait():
        for n, target in enumerate((kpool, vpool)):
            count = min(KH, KB - n * KH)
            if count > 0:
                spot = target.at[pl.ds(0, count * FB)]
                pltpu.make_async_copy(spot, spot, w_sem.at[3 + n]).wait()

    for copy in small:
        copy.start()
    for copy in kv_copies:
        copy.start()

    barrier = pltpu.get_barrier_semaphore()

    @pl.when(me > 0)
    def _():
        pl.semaphore_signal(barrier, inc=1, device_id={"dev": me - 1}, device_id_type=MESH)

    @pl.when(me < E)
    def _():
        pl.semaphore_signal(barrier, inc=1, device_id={"dev": me + 1}, device_id_type=MESH)

    for k in range(1, nc):
        pl.semaphore_signal(barrier, inc=1, device_id={"col": peer_of(k)}, device_id_type=MESH)

    small[2].wait()
    for n in range(heads):
        q_rows[pl.ds(n, B, stride=heads), :] = q_in[:, n * TILE : (n + 1) * TILE].astype(F32)
    small[0].wait()
    small[1].wait()
    def res_copy(k):
        spot = resid_all.at[pl.ds(pl.multiple_of(mc * R, R), R), :]
        return pltpu.make_async_remote_copy(
            src_ref=spot,
            dst_ref=spot,
            send_sem=res_s.at[k - 1],
            recv_sem=res_r.at[k - 1],
            device_id={"col": peer_of(k)},
            device_id_type=MESH,
        )

    neighbours = jnp.where(me > 0, 1, 0) + jnp.where(me < E, 1, 0)
    for copy in small[3:]:
        copy.wait()
    pl.semaphore_wait(barrier, neighbours + nc - 1)
    for k in range(1, nc):
        res_copy(k).start()
    kv_copies[0].wait()
    w_copies[0].start()

    PB = B // 2
    scale = TILE ** (-0.5)
    head_row = lax.broadcasted_iota(jnp.int32, (heads, TILE), 0) // group

    def blocked(value):
        if kvl == 1:
            return value.astype(BF16)
        wide = lax.broadcasted_iota(jnp.int32, value.shape, 0) // group
        return jnp.concatenate(
            [jnp.where(wide == h, value, 0.0).astype(BF16) for h in range(kvl)], axis=1
        )

    def att_copy(origin, a, way):
        spot = att_all.at[pl.ds(pl.multiple_of(origin * B + a * PB, PB), PB), :]
        return pltpu.make_async_remote_copy(
            src_ref=spot,
            dst_ref=spot,
            send_sem=att_s.at[way, origin, a],
            recv_sem=att_r.at[origin, a],
            device_id={"dev": me + (1 if way == 0 else -1)},
            device_id_type=MESH,
        )

    if True:
        @pl.loop(0, B // SUB)
        def _(b):
            for u in range(SUB):
                s = spot = b * SUB + u
                rows = pl.ds(pl.multiple_of(s * heads, heads), heads)
                query = blocked(q_rows[rows, :])
                keys = []
                for j in range(pages):
                    block = table[j, s]
                    keys.append(
                        jnp.concatenate([kpool[block * kvl + h] for h in range(kvl)], axis=1)
                        if kvl > 1
                        else kpool[block]
                    )
                value = lax.dot_general(
                    query,
                    jnp.concatenate(keys, axis=0),
                    (((1,), (1,)), ((), ())),
                    preferred_element_type=F32,
                ) * scale
                live = lax.broadcasted_iota(jnp.int32, value.shape, 1) < lens[s]
                scores[pl.ds(pl.multiple_of(spot * heads, heads), heads), :] = jnp.where(
                    live, value, -1e30
                )

    kv_copies[1].wait()
    w_copies[1].start()
    w_copies[2].start()
    for a in range(2):

        @pl.loop(0, PB // SUB)
        def _(b):
            base = a * PB + b * SUB
            rows = pl.ds(pl.multiple_of(base * heads, SUB * heads), SUB * heads)
            value = scores[rows, :]
            expo = jnp.exp(value - jnp.max(value, axis=1, keepdims=True))
            scores[rows, :] = expo / jnp.sum(expo, axis=1, keepdims=True)
            for u in range(SUB):
                spot = b * SUB + u
                s = a * PB + spot
                weights = blocked(scores[pl.ds(pl.multiple_of(s * heads, heads), heads), :])
                vals = [
                    vpool[table[j, s] * kvl + h]
                    for h in range(kvl)
                    for j in range(pages)
                ]
                o_rows[pl.ds(pl.multiple_of(spot * heads, heads), heads), :] = jnp.dot(
                    weights, jnp.concatenate(vals, axis=0), preferred_element_type=F32
                )

        mine = pl.ds(pl.multiple_of(me * B + a * PB, PB), PB)
        for n in range(heads):
            att_all[mine, n * TILE : (n + 1) * TILE] = o_rows[
                pl.ds(n, PB, stride=heads), :
            ].astype(BF16)

        @pl.when(me < E)
        def _():
            att_copy(me, a, 0).start()

        @pl.when(me > 0)
        def _():
            att_copy(me, a, 1).start()

    for n in range(KB):
        wd_copy(n).start()

    place = lax.broadcasted_iota(jnp.int32, (T, T), 0)
    position = place // R
    seat_here = ((position % NX) * 2 + position // NX) * R + place % R
    pick[...] = (seat_here == seat[...]).astype(F32).astype(BF16)
    fetch = (place == seat[...]).astype(F32).astype(BF16)

    def from_left(k, pass_on):
        for a in range(2):
            att_copy(me - k, a, 0).wait_recv()
            if pass_on:
                att_copy(me - k, a, 0).start()

    def from_right(k, pass_on):
        for a in range(2):
            att_copy(me + k, a, 1).wait_recv()
            if pass_on:
                att_copy(me + k, a, 1).start()

    def ends(k):
        @pl.when(jnp.logical_and(me == E, me - k >= 0))
        def _():
            from_left(k, False)

        @pl.when(jnp.logical_and(me == 0, me + k <= E))
        def _():
            from_right(k, False)

    def relay(k):
        @pl.when(jnp.logical_and(me < E, me - k >= 0))
        def _():
            from_left(k, True)

        @pl.when(jnp.logical_and(me > 0, me + k <= E))
        def _():
            from_right(k, True)

    @pl.loop(1, nd // 2)
    def _(k):
        relay(k)
        ends(k)

    half_rows = NX * RH

    def rows_of(step, c, x, count=1):
        start = halves[step] * half + (c * NX + x) * RH
        return pl.ds(pl.multiple_of(start, RH), count * RH)

    mid_own = pl.ds(pl.multiple_of(mx * RH, RH), RH)

    def whole(spot, send, recv):
        return pltpu.make_async_remote_copy(
            src_ref=spot,
            dst_ref=spot,
            send_sem=send,
            recv_sem=recv,
            device_id=partner,
            device_id_type=MESH,
        )

    def one_copy(step, j):
        cols = slice(j * WC, (j + 1) * WC)
        return pltpu.make_async_remote_copy(
            src_ref=proj.at[rows_of(step, 1 - core, 0, NX), cols],
            dst_ref=rs_one.at[step, :, cols],
            send_sem=one_s.at[step],
            recv_sem=one_r.at[step, j],
            device_id=partner,
            device_id_type=MESH,
        )

    def two_copy(step, k, j):
        cols = slice(j * WC, (j + 1) * WC)
        rows = pl.ds(pl.multiple_of(x_peer(k) * RH, RH), RH)
        return pltpu.make_async_remote_copy(
            src_ref=rs_mid.at[step, rows, cols],
            dst_ref=rs_two.at[step, k - 1, :, cols],
            send_sem=two_s.at[step, k - 1],
            recv_sem=two_r.at[step, k - 1, j],
            device_id={"col": x_peer(k) * 2 + core},
            device_id_type=MESH,
        )

    def project(step, j):
        cols = slice(j * WC, (j + 1) * WC)
        rows = pl.ds(pl.multiple_of(halves[step] * half, half), half)
        proj[rows, cols] = jnp.dot(
            att_all[rows, :], wo[:, cols], preferred_element_type=F32
        ).astype(BF16)
        one_copy(step, j).start()

    def meet(step, j):
        cols = slice(j * WC, (j + 1) * WC)
        one_copy(step, j).wait_recv()
        rs_mid[step, :, cols] = (
            proj[rows_of(step, core, 0, NX), cols].astype(F32) + rs_one[step, :, cols].astype(F32)
        ).astype(BF16)
        for k in range(1, NX):
            two_copy(step, k, j).start()

    def x_copy(step, k, j):
        spot = x_all.at[rows_of(step, core, mx), j * WC : (j + 1) * WC]
        return pltpu.make_async_remote_copy(
            src_ref=spot,
            dst_ref=spot,
            send_sem=x_s.at[step, k - 1],
            recv_sem=x_r.at[step, k - 1, j],
            device_id={"col": x_peer(k) * 2 + core},
            device_id_type=MESH,
        )

    def pair_copy(step, k, j):
        spot = x_all.at[rows_of(step, core, x_from(k)), j * WC : (j + 1) * WC]
        return pltpu.make_async_remote_copy(
            src_ref=spot,
            dst_ref=spot,
            send_sem=pair_s.at[step, k],
            recv_sem=pair_r.at[step],
            device_id=partner,
            device_id_type=MESH,
        )

    def streams(step):
        own_rows = rows_of(step, core, mx)
        for j in range(NJ):
            cols = slice(j * WC, (j + 1) * WC)
            value = (
                resid_rows[own_rows, cols].astype(F32)
                + proj[own_rows, cols].astype(F32)
                + rs_one[step, mid_own, cols].astype(F32)
            )
            for k in range(1, NX):
                two_copy(step, k, j).wait_recv()
                value = value + rs_two[step, k - 1, :, cols].astype(F32)
            stream[step, :, cols] = value
            x_all[own_rows, cols] = (value * gain[:, cols]).astype(BF16)
            for k in range(1, NX):
                x_copy(step, k, j).start()
            pair_copy(step, 0, j).start()

    def x_forward(step):
        for j in range(NJ):
            for k in range(1, NX):
                x_copy(step, k, j).wait_recv()
                pair_copy(step, k, j).start()

    def x_arrive(step):
        spot = x_all.at[rows_of(step, 1 - core, 0, NX), :]
        whole(spot, pair_s.at[step, 0], pair_r.at[step]).wait_recv()

    w_copies[0].wait()
    for j in range(NJ + 1):
        if j < NJ:
            project(0, j)
        if j > 0:
            meet(0, j - 1)

    @pl.loop(nd // 2, nd)
    def _(k):
        relay(k)

    for k in range(1, nc):
        res_copy(k).wait_recv()
    for j in range(NJ):
        cols = slice(j * WC, (j + 1) * WC)
        resid_rows[:, cols] = lax.dot_general(
            fetch, resid_all[:, cols], (((0,), (0,)), ((), ())), preferred_element_type=F32
        ).astype(BF16)
    streams(0)

    @pl.loop(nd // 2, nd)
    def _(k):
        ends(k)

    for j in range(NJ):
        project(1, j)
    x_forward(0)
    for j in range(NJ):
        meet(1, j)
    x_arrive(0)
    def neighbour(way):
        return {"dev": me + (1 if way == 0 else -1)}

    RQ = half // PART

    def sum_copy(way, c, r):
        rows = slice(r * RQ, (r + 1) * RQ)
        return pltpu.make_async_remote_copy(
            src_ref=own.at[c, way, rows, :],
            dst_ref=(in_r if way == 0 else in_l).at[c, rows, :],
            send_sem=sum_s.at[way],
            recv_sem=sum_r.at[way, c, r],
            device_id=neighbour(way),
            device_id_type=MESH,
        )

    def ssd_copy(way):
        return pltpu.make_async_remote_copy(
            src_ref=ss_own.at[pl.ds(way * half, half), :],
            dst_ref=ss_r if way == 0 else ss_l,
            send_sem=ssd_s.at[way],
            recv_sem=ssd_r.at[way],
            device_id=neighbour(way),
            device_id_type=MESH,
        )

    def hid_copy(way, c, r):
        spot = hid.at[c, pl.ds((1 - way) * half + r * RQ, RQ), :]
        return pltpu.make_async_remote_copy(
            src_ref=spot,
            dst_ref=spot,
            send_sem=hid_s.at[way],
            recv_sem=hid_r.at[way, c, r],
            device_id=neighbour(way),
            device_id_type=MESH,
        )

    def sum_stage(way, c):
        first = 0 if way == 0 else E
        last = E - first
        part = way
        incoming = in_r if way == 0 else in_l
        ss_in = ss_r if way == 0 else ss_l
        ss_rows = pl.ds(part * half, half)

        @pl.when(c == jnp.where(me == last, 0, min(1, NC - 1)))
        def _():
            ssd_copy(way).wait_recv()
            ss_own[ss_rows, :] = ss_own[ss_rows, :] + ss_in[...]

            @pl.when(me != last)
            def _():
                ssd_copy(way).start()

            @pl.when(me == last)
            def _():
                inv[...] = lax.rsqrt(ss_own[ss_rows, :] / full + 1e-5)

        for r in range(PART):
            rows = slice(r * RQ, (r + 1) * RQ)
            sum_copy(way, c, r).wait_recv()
            total = own[c, part, rows, :].astype(F32) + incoming[c, rows, :].astype(F32)

            @pl.when(me != last)
            def _():
                own[c, part, rows, :] = total.astype(BF16)
                sum_copy(way, c, r).start()

            @pl.when(me == last)
            def _():
                factor = inv[rows, 0:1]
                gate = total[:, :CF] * factor
                up = total[:, CF:] * factor
                hid[c, part * half + r * RQ : part * half + (r + 1) * RQ, :] = (
                    gate / (1.0 + jnp.exp(-gate)) * up
                ).astype(BF16)
                hid_copy(1 - way, c, r).start()

    def hid_stage(way, c):
        last = E if way == 0 else 0
        for r in range(PART):
            hid_copy(way, c, r).wait_recv()

            @pl.when(me != last)
            def _():
                hid_copy(way, c, r).start()

    def inside(c):
        return jnp.logical_and(c >= 0, c < NC)

    def sum_lag(d):
        return LAG_S0 + LAG_S * (d - 1)

    first_hid = max(NC + LAG_H0, sum_lag(E) + 1)

    def hid_lag(d):
        return first_hid + LAG_H * (d - 1)

    acc[...] = jnp.zeros_like(acc)
    w_copies[1].wait()
    w_copies[2].wait()

    @pl.loop(0, NC + hid_lag(E))
    def _(i):
        group = i // PHASE
        turn = halves[0] + group * (halves[1] - halves[0])
        turn_rows = pl.ds(pl.multiple_of(turn * half, half), half)

        @pl.when(i == min(LATER, PHASE))
        def _():
            streams(1)

        @pl.when(i == min(LATER + 3, PHASE))
        def _():
            x_forward(1)

        @pl.when(i == PHASE)
        def _():
            x_arrive(1)
        for p in range(PACE):
            q = (i - group * PHASE) * PACE + p

            @pl.when(jnp.logical_and(group < 2, q < NC))
            def _():
                cols = pl.ds(pl.multiple_of(q * CF, CF), CF)
                value = x_all[turn_rows, :]
                own[q, turn, :, :CF] = jnp.dot(
                    value, wg[:, cols], preferred_element_type=F32
                ).astype(BF16)
                own[q, turn, :, CF:] = jnp.dot(
                    value, wu[:, cols], preferred_element_type=F32
                ).astype(BF16)
                for way in (0, 1):
                    @pl.when(jnp.logical_and(group == 0, me == (0 if way == 0 else E)))
                    def _():
                        for r in range(PART):
                            sum_copy(way, q, r).start()

        @pl.when(jnp.logical_and(group < 2, i == group * PHASE))
        def _():
            squares = jnp.zeros((half, 1), F32)
            for j in range(NJ):
                cols = slice(j * WC, (j + 1) * WC)
                value = x_all[turn_rows, cols].astype(F32) / gain[:, cols]
                squares = squares + jnp.sum(value * value, axis=1, keepdims=True)
            ss_own[turn_rows, :] = jnp.broadcast_to(squares, (half, ss_own.shape[1]))
            for way in (0, 1):
                @pl.when(jnp.logical_and(group == 0, me == (0 if way == 0 else E)))
                def _():
                    ssd_copy(way).start()

        for way in (0, 1):
            d = me if way == 0 else E - me
            c = i - sum_lag(d)

            @pl.when(jnp.logical_and(d > 0, inside(c)))
            def _():
                sum_stage(way, c)

        for way in (0, 1):
            d = me if way == 0 else E - me
            c = i - hid_lag(d)

            @pl.when(jnp.logical_and(d > 0, inside(c)))
            def _():
                hid_stage(way, c)

        c = i - hid_lag(jnp.maximum(me, E - me))

        @pl.when(i == hid_lag(jnp.maximum(me, E - me)))
        def _():
            wd_wait()

        @pl.when(inside(c))
        def _():
            per = CF // TILE
            wide = 2 if KB % 2 == 0 else 1
            value = hid[c]
            for n in range(0, KB, wide):
                right = [
                    (kpool, vpool)[(n + w) // KH][
                        pl.ds((n + w) % KH * FB + c * per, per)
                    ].reshape(CF, TILE)
                    for w in range(wide)
                ]
                cols = slice(n * TILE, (n + wide) * TILE)
                acc[:, cols] += jnp.dot(
                    value, jnp.concatenate(right, axis=1), preferred_element_type=F32
                )

    my_half = pl.ds(pl.multiple_of(core * NX * R, R), NX * R)
    other_half = pl.ds(pl.multiple_of((1 - core) * NX * R, R), NX * R)

    def done_copy(j):
        cols = slice(j * WC, (j + 1) * WC)
        return pltpu.make_async_remote_copy(
            src_ref=down.at[other_half, cols],
            dst_ref=dn_one.at[:, cols],
            send_sem=done_s.at[0],
            recv_sem=done_r.at[j],
            device_id=partner,
            device_id_type=MESH,
        )

    def last_copy(k, j):
        cols = slice(j * WC, (j + 1) * WC)
        rows = pl.ds(pl.multiple_of(x_peer(k) * R, R), R)
        return pltpu.make_async_remote_copy(
            src_ref=dn_mid.at[rows, cols],
            dst_ref=dn_two.at[k - 1, :, cols],
            send_sem=dtwo_s.at[k - 1],
            recv_sem=dtwo_r.at[k - 1, j],
            device_id={"col": x_peer(k) * 2 + core},
            device_id_type=MESH,
        )

    for step in (0, 1):
        rows = rows_of(step, core, mx)
        acc[rows, :] = acc[rows, :] + stream[step]
    for j in range(NJ + 1):
        if j < NJ:
            cols = slice(j * WC, (j + 1) * WC)
            down[:, cols] = jnp.dot(
                pick[...], acc[:, cols].astype(BF16), preferred_element_type=F32
            ).astype(BF16)
            done_copy(j).start()
        if j > 0:
            cols = slice((j - 1) * WC, j * WC)
            done_copy(j - 1).wait_recv()
            dn_mid[:, cols] = (
                down[my_half, cols].astype(F32) + dn_one[:, cols].astype(F32)
            ).astype(BF16)
            for k in range(1, NX):
                last_copy(k, j - 1).start()
    my_rows = pl.ds(pl.multiple_of((core * NX + mx) * R, R), R)
    my_mid = pl.ds(pl.multiple_of(mx * R, R), R)
    for j in range(NJ):
        cols = slice(j * WC, (j + 1) * WC)
        value = down[my_rows, cols].astype(F32) + dn_one[my_mid, cols].astype(F32)
        for k in range(1, NX):
            last_copy(k, j).wait_recv()
            value = value + dn_two[k - 1, :, cols].astype(F32)
        out[:, cols] = value.astype(BF16)

    for k in range(1, nc):
        res_copy(k).wait_send()
    for step in (0, 1):
        mine = x_all.at[rows_of(step, core, mx), :]
        whole(proj.at[rows_of(step, 1 - core, 0, NX), :], one_s.at[step], one_r.at[step, 0]).wait_send()
        for k in range(1, NX):
            whole(mine, two_s.at[step, k - 1], one_r.at[step, 0]).wait_send()
            whole(mine, x_s.at[step, k - 1], one_r.at[step, 0]).wait_send()
        for k in range(NX):
            whole(mine, pair_s.at[step, k], one_r.at[step, 0]).wait_send()
    whole(down.at[other_half, :], done_s.at[0], done_r.at[0]).wait_send()
    for k in range(1, NX):
        whole(down.at[my_rows, :], dtwo_s.at[k - 1], done_r.at[0]).wait_send()

    for a in range(2):
        @pl.loop(0, nd)
        def _(origin):
            @pl.when(jnp.logical_and(me < E, origin <= me))
            def _():
                att_copy(origin, a, 0).wait_send()

            @pl.when(jnp.logical_and(me > 0, origin >= me))
            def _():
                att_copy(origin, a, 1).wait_send()

    for way in (0, 1):
        @pl.when(me != (E if way == 0 else 0))
        def _():
            ssd_copy(way).wait_send()

            whole(own.at[:, way], sum_s.at[way], sum_r.at[way, 0, 0]).wait_send()
            sent = hid.at[:, pl.ds((1 - way) * half, half), :]
            whole(sent, hid_s.at[way], hid_r.at[way, 0, 0]).wait_send()


def solution(mesh):
    nd, nc = mesh.shape["dev"], mesh.shape["col"]

    def on_device(
        queries,
        kv_pages,
        page_table,
        seq_lengths,
        ffn_seat,
        resid,
        w_out,
        norm_gain,
        w_gate,
        w_up,
        w_down,
    ):
        B, HK = queries.shape
        blocks, kvl, _, page, head_dim = kv_pages.shape
        pages = page_table.shape[1]
        group = HK // (kvl * head_dim)
        heads = kvl * group
        T = ffn_seat.shape[0]
        R, DK = resid.shape
        FK = w_gate.shape[1]
        WC = divisor(DK, (WCM, 512, 256, 128))
        NJ = DK // WC
        CF = divisor(FK, (256, 128))
        NC = FK // CF
        half = T // 2
        NX = nc // 2
        KB, FB = DK // TILE, FK // TILE
        dims = (
            T, B, R, HK, DK, FK, kvl, group, pages, blocks, WC, NJ, CF, NC, half, NX, float(DK * nd)
        )
        dma = pltpu.SemaphoreType.DMA
        hbm = pl.BlockSpec(memory_space=pltpu.HBM)
        vmem = pltpu.VMEM
        PB = B // 2
        scratch = [
            pltpu.SMEM((pages, B), jnp.int32),
            pltpu.SMEM((B,), jnp.int32),
            vmem((B, HK), BF16),
            vmem((1, T), jnp.int32),
            vmem((T, DK), BF16),
            vmem((T, DK), BF16),
            vmem((T, T), BF16),
            vmem((1, DK), F32),
            vmem((HK, DK), BF16),
            vmem((DK, FK), BF16),
            vmem((DK, FK), BF16),
            vmem((max(blocks * kvl, (KB + 1) // 2 * FB), TILE, TILE), BF16),
            vmem((max(blocks * kvl, (KB + 1) // 2 * FB), TILE, TILE), BF16),
            vmem((B * heads, head_dim), F32),
            vmem((PB * heads, head_dim), F32),
            vmem((B * heads, pages * page), F32),
            vmem((T, HK), BF16),
            vmem((T, DK), BF16),
            vmem((2, half // 2, DK), BF16),
            vmem((2, half // 2, DK), BF16),
            vmem((2, max(NX - 1, 1), half // nc, DK), BF16),
            vmem((T, DK), BF16),
            vmem((2, half // nc, DK), F32),
            vmem((NC, 2, half, 2 * CF), BF16),
            vmem((NC, half, 2 * CF), BF16),
            vmem((NC, half, 2 * CF), BF16),
            vmem((T, 128), F32),
            vmem((half, 128), F32),
            vmem((half, 128), F32),
            vmem((half, 128), F32),
            vmem((NC, T, CF), BF16),
            vmem((T, DK), F32),
            vmem((T, DK), BF16),
            vmem((NX * R, DK), BF16),
            vmem((NX * R, DK), BF16),
            vmem((max(NX - 1, 1), R, DK), BF16),
            dma((6,)),
            dma((2,)),
            dma((5,)),
            dma((2, nd, 2)),
            dma((nd, 2)),
            dma((nc - 1,)),
            dma((nc - 1,)),
            dma((2,)),
            dma((2, NJ)),
            dma((2, max(NX - 1, 1))),
            dma((2, max(NX - 1, 1), NJ)),
            dma((2, max(NX - 1, 1))),
            dma((2, max(NX - 1, 1), NJ)),
            dma((2, NX)),
            dma((2,)),
            dma((2,)),
            dma((2, NC, PART)),
            dma((2,)),
            dma((2,)),
            dma((2,)),
            dma((2, NC, PART)),
            dma((1,)),
            dma((NJ,)),
            dma((max(NX - 1, 1),)),
            dma((max(NX - 1, 1), NJ)),
        ]
        return pl.pallas_call(
            functools.partial(layer_kernel, nd, nc, dims),
            out_shape=pltpu.VMEM((R, DK), BF16),
            in_specs=[hbm] * 11,
            out_specs=pl.BlockSpec(memory_space=pltpu.VMEM),
            scratch_shapes=scratch,
            compiler_params=pltpu.CompilerParams(
                collective_id=0, has_side_effects=True, vmem_limit_bytes=65 * 1000 * 1000
            ),
        )(
            page_table.T,
            seq_lengths,
            queries,
            kv_pages.reshape(blocks * kvl, 2, page, head_dim),
            ffn_seat[None, :],
            resid,
            norm_gain[None, :],
            w_out,
            w_gate,
            w_up,
            w_down.reshape(FB, TILE, DK),
        )

    in_specs = (
        P(("rep", "dev"), "col"),
        P(("rep", "dev"), "col", None, None, None),
        P(("rep", "dev"), None),
        P(("rep", "dev")),
        P("rep"),
        P(("rep", "col"), "dev"),
        P("col", "dev"),
        P("dev"),
        P("dev", "col"),
        P("dev", "col"),
        P("col", "dev"),
    )
    return jax.shard_map(
        on_device,
        mesh=mesh,
        in_specs=in_specs,
        out_specs=P(("rep", "col"), "dev"),
        check_vma=False,
    )
```

```python
import functools

import jax
import jax.numpy as jnp
from jax import lax
from jax.experimental import pallas as pl
from jax.experimental.pallas import tpu as pltpu
from jax.sharding import PartitionSpec as P

MESH = pl.DeviceIdType.MESH
F32 = jnp.float32
BF16 = jnp.bfloat16
TILE = 128
SUB = 8
LATER = 5
END_PROJ = 2
END_GAP = 2
PART = 1
WCM = 1024
LAG_S0 = 4
LAG_S = 3
LAG_H0 = 4
LAG_H = 5


def divisor(size, choices):
    for choice in choices:
        if size % choice == 0:
            return choice
    return size


def layer_kernel(
    nd,
    nc,
    dims,
    table_hbm,
    len_hbm,
    q_hbm,
    kv_hbm,
    seat_hbm,
    resid_hbm,
    gain_hbm,
    wo_hbm,
    wg_hbm,
    wu_hbm,
    wd_hbm,
    out,
    table,
    lens,
    q_in,
    seat,
    resid_all,
    resid_rows,
    pick,
    gain,
    wo,
    wg,
    wu,
    kpool,
    vpool,
    q_rows,
    o_rows,
    scores,
    att_all,
    proj,
    rs_one,
    rs_mid,
    rs_two,
    x_all,
    stream,
    own,
    in_r,
    in_l,
    ss_own,
    ss_r,
    ss_l,
    inv,
    hid,
    acc,
    dn_one,
    dn_mid,
    dn_two,
    in_sem,
    kv_sem,
    w_sem,
    att_s,
    att_r,
    far_s,
    res_s,
    res_r,
    one_s,
    one_r,
    two_s,
    two_r,
    pair_s,
    pair_r,
    sum_s,
    sum_r,
    ssd_s,
    ssd_r,
    hid_s,
    hid_r,
    done_s,
    done_r,
    dtwo_s,
    dtwo_r,
):
    T, B, R, HK, DK, FK, kvl, group, pages, blocks, WC, NJ, CF, NC, half, NX, full = dims
    RH = half // nc
    PACE = 2 if NC % 2 == 0 else 1
    PHASE = NC // PACE
    MID_START = max(PHASE, LATER + 2)
    END_START = MID_START + END_GAP
    me = lax.axis_index("dev")
    mc = lax.axis_index("col")
    mx, core = mc // 2, mc % 2
    E = nd - 1
    late_dev = (me * 2) // nd
    halves = (late_dev, 1 - late_dev)
    heads = kvl * group
    span = pages * TILE
    KB = DK // TILE
    FB = FK // TILE
    KH = (KB + 1) // 2
    partner = {"col": mx * 2 + 1 - core}

    def peer_of(k):
        return lax.rem(mc + k, nc)

    def x_peer(k):
        return lax.rem(mx + k, NX)

    def x_from(k):
        return lax.rem(mx + NX - k, NX)

    small = [
        pltpu.make_async_copy(table_hbm, table, in_sem.at[0]),
        pltpu.make_async_copy(len_hbm, lens, in_sem.at[1]),
        pltpu.make_async_copy(q_hbm, q_in, in_sem.at[2]),
        pltpu.make_async_copy(seat_hbm, seat, in_sem.at[3]),
        pltpu.make_async_copy(
            resid_hbm, resid_all.at[pl.ds(pl.multiple_of(mc * R, R), R), :], in_sem.at[4]
        ),
        pltpu.make_async_copy(gain_hbm, gain, in_sem.at[5]),
    ]
    kv_count = blocks * kvl
    kv_copies = [
        pltpu.make_async_copy(
            kv_hbm.at[:, v], (kpool, vpool)[v].at[pl.ds(0, kv_count)], kv_sem.at[v]
        )
        for v in (0, 1)
    ]
    w_copies = [
        pltpu.make_async_copy(wo_hbm, wo, w_sem.at[0]),
        pltpu.make_async_copy(wg_hbm, wg, w_sem.at[1]),
        pltpu.make_async_copy(wu_hbm, wu, w_sem.at[2]),
    ]

    def wd_copy(n):
        cols = slice(n * TILE, (n + 1) * TILE)
        return pltpu.make_async_copy(
            wd_hbm.at[:, :, cols],
            (kpool, vpool)[n // KH].at[pl.ds(n % KH * FB, FB)],
            w_sem.at[3 + n // KH],
        )

    def wd_wait():
        for n, target in enumerate((kpool, vpool)):
            count = min(KH, KB - n * KH)
            if count > 0:
                spot = target.at[pl.ds(0, count * FB)]
                pltpu.make_async_copy(spot, spot, w_sem.at[3 + n]).wait()

    for copy in small:
        copy.start()
    for copy in kv_copies:
        copy.start()

    barrier = pltpu.get_barrier_semaphore()

    @pl.when(me > 0)
    def _():
        pl.semaphore_signal(barrier, inc=1, device_id={"dev": me - 1}, device_id_type=MESH)

    @pl.when(me < E)
    def _():
        pl.semaphore_signal(barrier, inc=1, device_id={"dev": me + 1}, device_id_type=MESH)

    for here, there in ((E - 2, E), (E, E - 2), (2, 0), (0, 2)):
        @pl.when(me == here)
        def _():
            pl.semaphore_signal(barrier, inc=1, device_id={"dev": there}, device_id_type=MESH)

    for k in range(1, nc):
        pl.semaphore_signal(barrier, inc=1, device_id={"col": peer_of(k)}, device_id_type=MESH)

    small[2].wait()
    for n in range(heads):
        q_rows[pl.ds(n, B, stride=heads), :] = q_in[:, n * TILE : (n + 1) * TILE].astype(F32)
    small[0].wait()
    small[1].wait()
    def res_copy(k):
        spot = resid_all.at[pl.ds(pl.multiple_of(mc * R, R), R), :]
        return pltpu.make_async_remote_copy(
            src_ref=spot,
            dst_ref=spot,
            send_sem=res_s.at[k - 1],
            recv_sem=res_r.at[k - 1],
            device_id={"col": peer_of(k)},
            device_id_type=MESH,
        )

    neighbours = jnp.where(me > 0, 1, 0) + jnp.where(me < E, 1, 0)
    for here in (E - 2, E, 2, 0):
        neighbours = neighbours + jnp.where(me == here, 1, 0)
    for copy in small[3:]:
        copy.wait()
    pl.semaphore_wait(barrier, neighbours + nc - 1)
    for k in range(1, nc):
        res_copy(k).start()
    kv_copies[0].wait()
    w_copies[0].start()

    PB = B // 2
    scale = TILE ** (-0.5)
    head_row = lax.broadcasted_iota(jnp.int32, (heads, TILE), 0) // group

    def blocked(value):
        if kvl == 1:
            return value.astype(BF16)
        wide = lax.broadcasted_iota(jnp.int32, value.shape, 0) // group
        return jnp.concatenate(
            [jnp.where(wide == h, value, 0.0).astype(BF16) for h in range(kvl)], axis=1
        )

    def att_copy(origin, a, way):
        spot = att_all.at[pl.ds(pl.multiple_of(origin * B + a * PB, PB), PB), :]
        return pltpu.make_async_remote_copy(
            src_ref=spot,
            dst_ref=spot,
            send_sem=att_s.at[way, origin, a],
            recv_sem=att_r.at[origin, a],
            device_id={"dev": me + (1 if way == 0 else -1)},
            device_id_type=MESH,
        )

    if True:
        @pl.loop(0, B // SUB)
        def _(b):
            for u in range(SUB):
                s = spot = b * SUB + u
                rows = pl.ds(pl.multiple_of(s * heads, heads), heads)
                query = blocked(q_rows[rows, :])
                keys = []
                for j in range(pages):
                    block = table[j, s]
                    keys.append(
                        jnp.concatenate([kpool[block * kvl + h] for h in range(kvl)], axis=1)
                        if kvl > 1
                        else kpool[block]
                    )
                value = lax.dot_general(
                    query,
                    jnp.concatenate(keys, axis=0),
                    (((1,), (1,)), ((), ())),
                    preferred_element_type=F32,
                ) * scale
                live = lax.broadcasted_iota(jnp.int32, value.shape, 1) < lens[s]
                scores[pl.ds(pl.multiple_of(spot * heads, heads), heads), :] = jnp.where(
                    live, value, -1e30
                )

    kv_copies[1].wait()
    w_copies[1].start()
    w_copies[2].start()
    def far_copy(way, a):
        origin = 0 if way == 0 else E
        spot = att_all.at[pl.ds(origin * B + a * PB, PB), :]
        return pltpu.make_async_remote_copy(
            src_ref=spot,
            dst_ref=spot,
            send_sem=far_s.at[way, a],
            recv_sem=att_r.at[origin, a],
            device_id={"dev": E - origin},
            device_id_type=MESH,
        )

    for a in range(2):

        @pl.loop(0, PB // SUB)
        def _(b):
            base = a * PB + b * SUB
            rows = pl.ds(pl.multiple_of(base * heads, SUB * heads), SUB * heads)
            value = scores[rows, :]
            expo = jnp.exp(value - jnp.max(value, axis=1, keepdims=True))
            scores[rows, :] = expo / jnp.sum(expo, axis=1, keepdims=True)
            for u in range(SUB):
                spot = b * SUB + u
                s = a * PB + spot
                weights = blocked(scores[pl.ds(pl.multiple_of(s * heads, heads), heads), :])
                vals = [
                    vpool[table[j, s] * kvl + h]
                    for h in range(kvl)
                    for j in range(pages)
                ]
                o_rows[pl.ds(pl.multiple_of(spot * heads, heads), heads), :] = jnp.dot(
                    weights, jnp.concatenate(vals, axis=0), preferred_element_type=F32
                )

        mine = pl.ds(pl.multiple_of(me * B + a * PB, PB), PB)
        for n in range(heads):
            att_all[mine, n * TILE : (n + 1) * TILE] = o_rows[
                pl.ds(n, PB, stride=heads), :
            ].astype(BF16)

        @pl.when(me < E)
        def _():
            att_copy(me, a, 0).start()

        @pl.when(me > 0)
        def _():
            att_copy(me, a, 1).start()

    for n in range(KB):
        wd_copy(n).start()

    place = lax.broadcasted_iota(jnp.int32, (T, T), 0)
    position = place // R
    seat_here = ((position % NX) * 2 + position // NX) * R + place % R
    pick[...] = (seat_here == seat[...]).astype(F32).astype(BF16)
    fetch = (place == seat[...]).astype(F32).astype(BF16)

    def passes(origin, way):
        if way == 0:
            return jnp.logical_and(me < E, jnp.logical_or(origin > 0, me + 1 < E))
        return jnp.logical_and(me > 0, jnp.logical_or(origin < E, me - 1 > 0))

    def take(origin, way, relay):
        inside = origin >= 0 if way == 0 else origin <= E
        move = passes(origin, way)
        wanted = move if relay else jnp.logical_not(move)

        @pl.when(jnp.logical_and(inside, wanted))
        def _():
            for a in range(2):
                att_copy(origin, a, way).wait_recv()
                if relay:
                    att_copy(origin, a, way).start()

                    @pl.when(
                        jnp.logical_and(
                            me == (E - 2 if way == 0 else 2), origin == (0 if way == 0 else E)
                        )
                    )
                    def _():
                        far_copy(way, a).start()

    def both(k, relay):
        take(me - k, 0, relay)
        take(me + k, 1, relay)

    @pl.loop(1, nd // 2)
    def _(k):
        both(k, True)
        both(k, False)

    half_rows = NX * RH

    def rows_of(step, c, x, count=1):
        start = halves[step] * half + (c * NX + x) * RH
        return pl.ds(pl.multiple_of(start, RH), count * RH)

    mid_own = pl.ds(pl.multiple_of(mx * RH, RH), RH)

    def whole(spot, send, recv):
        return pltpu.make_async_remote_copy(
            src_ref=spot,
            dst_ref=spot,
            send_sem=send,
            recv_sem=recv,
            device_id=partner,
            device_id_type=MESH,
        )

    def one_copy(step, j):
        cols = slice(j * WC, (j + 1) * WC)
        return pltpu.make_async_remote_copy(
            src_ref=proj.at[rows_of(step, 1 - core, 0, NX), cols],
            dst_ref=rs_one.at[step, :, cols],
            send_sem=one_s.at[step],
            recv_sem=one_r.at[step, j],
            device_id=partner,
            device_id_type=MESH,
        )

    def two_copy(step, k, j):
        cols = slice(j * WC, (j + 1) * WC)
        return pltpu.make_async_remote_copy(
            src_ref=rs_mid.at[step, :, cols],
            dst_ref=rs_two.at[step, k - 1, :, cols],
            send_sem=two_s.at[step, k - 1],
            recv_sem=two_r.at[step, k - 1, j],
            device_id={"col": x_peer(k) * 2 + core},
            device_id_type=MESH,
        )

    def project(step, j):
        cols = slice(j * WC, (j + 1) * WC)
        rows = pl.ds(pl.multiple_of(halves[step] * half, half), half)
        proj[rows, cols] = jnp.dot(
            att_all[rows, :], wo[:, cols], preferred_element_type=F32
        ).astype(BF16)
        one_copy(step, j).start()

    def meet(step, j):
        cols = slice(j * WC, (j + 1) * WC)
        one_copy(step, j).wait_recv()
        rs_mid[step, :, cols] = (
            proj[rows_of(step, core, 0, NX), cols].astype(F32) + rs_one[step, :, cols].astype(F32)
        ).astype(BF16)
        for k in range(1, NX):
            two_copy(step, k, j).start()

    def pair_copy(step, j):
        spot = x_all.at[rows_of(step, core, 0, NX), j * WC : (j + 1) * WC]
        return pltpu.make_async_remote_copy(
            src_ref=spot,
            dst_ref=spot,
            send_sem=pair_s.at[step],
            recv_sem=pair_r.at[step],
            device_id=partner,
            device_id_type=MESH,
        )

    def streams(step):
        rows = rows_of(step, core, 0, NX)
        for j in range(NJ):
            cols = slice(j * WC, (j + 1) * WC)
            value = (
                resid_rows[rows, cols].astype(F32)
                + proj[rows, cols].astype(F32)
                + rs_one[step, :, cols].astype(F32)
            )
            for k in range(1, NX):
                two_copy(step, k, j).wait_recv()
                value = value + rs_two[step, k - 1, :, cols].astype(F32)
            stream[step, :, cols] = value
            x_all[rows, cols] = (value * gain[:, cols]).astype(BF16)
            pair_copy(step, j).start()

    def x_arrive(step):
        spot = x_all.at[rows_of(step, 1 - core, 0, NX), :]
        whole(spot, pair_s.at[step], pair_r.at[step]).wait_recv()

    w_copies[0].wait()
    for j in range(NJ + 1):
        if j < NJ:
            project(0, j)
        if j > 0:
            meet(0, j - 1)

    @pl.loop(nd // 2, nd)
    def _(k):
        both(k, True)

    for k in range(1, nc):
        res_copy(k).wait_recv()
    for j in range(NJ):
        cols = slice(j * WC, (j + 1) * WC)
        resid_rows[:, cols] = lax.dot_general(
            fetch, resid_all[:, cols], (((0,), (0,)), ((), ())), preferred_element_type=F32
        ).astype(BF16)

    is_end = jnp.logical_or(me == 0, me == E)

    def second_part():
        @pl.loop(nd // 2, nd)
        def _(k):
            both(k, False)

        for j in range(NJ):
            project(1, j)

    @pl.when(jnp.logical_not(is_end))
    def _():
        second_part()

    streams(0)

    @pl.when(jnp.logical_not(is_end))
    def _():
        for j in range(NJ):
            meet(1, j)

    x_arrive(0)
    def neighbour(way):
        return {"dev": me + (1 if way == 0 else -1)}

    RQ = half // PART

    def sum_copy(way, c, r):
        rows = slice(r * RQ, (r + 1) * RQ)
        return pltpu.make_async_remote_copy(
            src_ref=own.at[c, way, rows, :],
            dst_ref=(in_r if way == 0 else in_l).at[c, rows, :],
            send_sem=sum_s.at[way],
            recv_sem=sum_r.at[way, c, r],
            device_id=neighbour(way),
            device_id_type=MESH,
        )

    def ssd_copy(way):
        return pltpu.make_async_remote_copy(
            src_ref=ss_own.at[pl.ds(way * half, half), :],
            dst_ref=ss_r if way == 0 else ss_l,
            send_sem=ssd_s.at[way],
            recv_sem=ssd_r.at[way],
            device_id=neighbour(way),
            device_id_type=MESH,
        )

    def hid_copy(way, c, r):
        spot = hid.at[c, pl.ds((1 - way) * half + r * RQ, RQ), :]
        return pltpu.make_async_remote_copy(
            src_ref=spot,
            dst_ref=spot,
            send_sem=hid_s.at[way],
            recv_sem=hid_r.at[way, c, r],
            device_id=neighbour(way),
            device_id_type=MESH,
        )

    def sum_stage(way, c):
        first = 0 if way == 0 else E
        last = E - first
        part = way
        incoming = in_r if way == 0 else in_l
        ss_in = ss_r if way == 0 else ss_l
        ss_rows = pl.ds(part * half, half)

        @pl.when(c == jnp.where(me == last, 0, min(1, NC - 1)))
        def _():
            ssd_copy(way).wait_recv()
            ss_own[ss_rows, :] = ss_own[ss_rows, :] + ss_in[...]

            @pl.when(me != last)
            def _():
                ssd_copy(way).start()

            @pl.when(me == last)
            def _():
                inv[...] = lax.rsqrt(ss_own[ss_rows, :] / full + 1e-5)

        for r in range(PART):
            rows = slice(r * RQ, (r + 1) * RQ)
            sum_copy(way, c, r).wait_recv()
            total = own[c, part, rows, :].astype(F32) + incoming[c, rows, :].astype(F32)

            @pl.when(me != last)
            def _():
                own[c, part, rows, :] = total.astype(BF16)
                sum_copy(way, c, r).start()

            @pl.when(me == last)
            def _():
                factor = inv[rows, 0:1]
                gate = total[:, :CF] * factor
                up = total[:, CF:] * factor
                hid[c, part * half + r * RQ : part * half + (r + 1) * RQ, :] = (
                    gate / (1.0 + jnp.exp(-gate)) * up
                ).astype(BF16)
                hid_copy(1 - way, c, r).start()

    def hid_stage(way, c):
        last = E if way == 0 else 0
        for r in range(PART):
            hid_copy(way, c, r).wait_recv()

            @pl.when(me != last)
            def _():
                hid_copy(way, c, r).start()

    def inside(c):
        return jnp.logical_and(c >= 0, c < NC)

    def sum_lag(d):
        return LAG_S0 + LAG_S * (d - 1)

    first_hid = max(NC + LAG_H0, sum_lag(E) + 1)

    def hid_lag(d):
        return first_hid + LAG_H * (d - 1)

    acc[...] = jnp.zeros_like(acc)
    w_copies[1].wait()
    w_copies[2].wait()

    second_start = jnp.where(is_end, END_START, MID_START)

    @pl.loop(0, NC + hid_lag(E))
    def _(i):
        again = i >= second_start
        turn = jnp.where(again, halves[1], halves[0])
        turn_rows = pl.ds(pl.multiple_of(turn * half, half), half)
        place_in = jnp.where(again, i - second_start, i)

        @pl.when(jnp.logical_and(is_end, i == END_PROJ))
        def _():
            second_part()

        @pl.when(jnp.logical_and(is_end, i == END_PROJ + 2))
        def _():
            for j in range(NJ):
                meet(1, j)

        @pl.when(i == jnp.where(is_end, END_START - 1, LATER))
        def _():
            streams(1)

        @pl.when(i == second_start)
        def _():
            x_arrive(1)
        @pl.when(place_in < PHASE)
        def _():
            value = x_all[turn_rows, :]
            for p in range(PACE):
                q = place_in * PACE + p
                cols = pl.ds(pl.multiple_of(q * CF, CF), CF)
                own[q, turn, :, :CF] = jnp.dot(
                    value, wg[:, cols], preferred_element_type=F32
                ).astype(BF16)
                own[q, turn, :, CF:] = jnp.dot(
                    value, wu[:, cols], preferred_element_type=F32
                ).astype(BF16)

        for way in (0, 1):
            @pl.when(jnp.logical_and(i < PHASE, me == (0 if way == 0 else E)))
            def _():
                for p in range(PACE):
                    for r in range(PART):
                        sum_copy(way, i * PACE + p, r).start()

        @pl.when(place_in == 0)
        def _():
            squares = jnp.zeros((half, 1), F32)
            for j in range(NJ):
                cols = slice(j * WC, (j + 1) * WC)
                value = x_all[turn_rows, cols].astype(F32) / gain[:, cols]
                squares = squares + jnp.sum(value * value, axis=1, keepdims=True)
            ss_own[turn_rows, :] = jnp.broadcast_to(squares, (half, ss_own.shape[1]))
            for way in (0, 1):
                @pl.when(jnp.logical_and(i == 0, me == (0 if way == 0 else E)))
                def _():
                    ssd_copy(way).start()

        for way in (0, 1):
            d = me if way == 0 else E - me
            c = i - sum_lag(d)

            @pl.when(jnp.logical_and(d > 0, inside(c)))
            def _():
                sum_stage(way, c)

        for way in (0, 1):
            d = me if way == 0 else E - me
            c = i - hid_lag(d)

            @pl.when(jnp.logical_and(d > 0, inside(c)))
            def _():
                hid_stage(way, c)

        c = i - hid_lag(jnp.maximum(me, E - me))

        @pl.when(i == hid_lag(jnp.maximum(me, E - me)))
        def _():
            wd_wait()

        @pl.when(inside(c))
        def _():
            per = CF // TILE
            wide = 2 if KB % 2 == 0 else 1
            value = hid[c]
            for n in range(0, KB, wide):
                right = [
                    (kpool, vpool)[(n + w) // KH][
                        pl.ds((n + w) % KH * FB + c * per, per)
                    ].reshape(CF, TILE)
                    for w in range(wide)
                ]
                cols = slice(n * TILE, (n + wide) * TILE)
                acc[:, cols] += jnp.dot(
                    value, jnp.concatenate(right, axis=1), preferred_element_type=F32
                )

    down = resid_rows
    my_half = pl.ds(pl.multiple_of(core * NX * R, R), NX * R)
    other_half = pl.ds(pl.multiple_of((1 - core) * NX * R, R), NX * R)

    def done_copy(j):
        cols = slice(j * WC, (j + 1) * WC)
        return pltpu.make_async_remote_copy(
            src_ref=down.at[other_half, cols],
            dst_ref=dn_one.at[:, cols],
            send_sem=done_s.at[0],
            recv_sem=done_r.at[j],
            device_id=partner,
            device_id_type=MESH,
        )

    def last_copy(k, j):
        cols = slice(j * WC, (j + 1) * WC)
        rows = pl.ds(pl.multiple_of(x_peer(k) * R, R), R)
        return pltpu.make_async_remote_copy(
            src_ref=dn_mid.at[rows, cols],
            dst_ref=dn_two.at[k - 1, :, cols],
            send_sem=dtwo_s.at[k - 1],
            recv_sem=dtwo_r.at[k - 1, j],
            device_id={"col": x_peer(k) * 2 + core},
            device_id_type=MESH,
        )

    for step in (0, 1):
        rows = rows_of(step, core, mx)
        acc[rows, :] = acc[rows, :] + stream[step, mid_own, :]
    for j in range(NJ + 1):
        if j < NJ:
            cols = slice(j * WC, (j + 1) * WC)
            down[:, cols] = jnp.dot(
                pick[...], acc[:, cols].astype(BF16), preferred_element_type=F32
            ).astype(BF16)
            done_copy(j).start()
        if j > 0:
            cols = slice((j - 1) * WC, j * WC)
            done_copy(j - 1).wait_recv()
            dn_mid[:, cols] = (
                down[my_half, cols].astype(F32) + dn_one[:, cols].astype(F32)
            ).astype(BF16)
            for k in range(1, NX):
                last_copy(k, j - 1).start()
    my_rows = pl.ds(pl.multiple_of((core * NX + mx) * R, R), R)
    my_mid = pl.ds(pl.multiple_of(mx * R, R), R)
    for j in range(NJ):
        cols = slice(j * WC, (j + 1) * WC)
        value = down[my_rows, cols].astype(F32) + dn_one[my_mid, cols].astype(F32)
        for k in range(1, NX):
            last_copy(k, j).wait_recv()
            value = value + dn_two[k - 1, :, cols].astype(F32)
        out[:, cols] = value.astype(BF16)

    for k in range(1, nc):
        res_copy(k).wait_send()
    for step in (0, 1):
        mine = x_all.at[rows_of(step, core, 0, NX), :]
        whole(proj.at[rows_of(step, 1 - core, 0, NX), :], one_s.at[step], one_r.at[step, 0]).wait_send()
        for k in range(1, NX):
            whole(mine, two_s.at[step, k - 1], one_r.at[step, 0]).wait_send()
        whole(mine, pair_s.at[step], one_r.at[step, 0]).wait_send()
    whole(down.at[other_half, :], done_s.at[0], done_r.at[0]).wait_send()
    for k in range(1, NX):
        whole(down.at[my_rows, :], dtwo_s.at[k - 1], done_r.at[0]).wait_send()

    for way in (0, 1):
        @pl.when(me == (E - 2 if way == 0 else 2))
        def _():
            for a in range(2):
                far_copy(way, a).wait_send()

    for a in range(2):
        @pl.loop(0, nd)
        def _(origin):
            left = jnp.logical_or(origin == me, jnp.logical_and(origin < me, passes(origin, 0)))
            right = jnp.logical_or(origin == me, jnp.logical_and(origin > me, passes(origin, 1)))

            @pl.when(jnp.logical_and(me < E, left))
            def _():
                att_copy(origin, a, 0).wait_send()

            @pl.when(jnp.logical_and(me > 0, right))
            def _():
                att_copy(origin, a, 1).wait_send()

    for way in (0, 1):
        @pl.when(me != (E if way == 0 else 0))
        def _():
            ssd_copy(way).wait_send()

            whole(own.at[:, way], sum_s.at[way], sum_r.at[way, 0, 0]).wait_send()
            sent = hid.at[:, pl.ds((1 - way) * half, half), :]
            whole(sent, hid_s.at[way], hid_r.at[way, 0, 0]).wait_send()


def solution(mesh):
    nd, nc = mesh.shape["dev"], mesh.shape["col"]

    def on_device(
        queries,
        kv_pages,
        page_table,
        seq_lengths,
        ffn_seat,
        resid,
        w_out,
        norm_gain,
        w_gate,
        w_up,
        w_down,
    ):
        B, HK = queries.shape
        blocks, kvl, _, page, head_dim = kv_pages.shape
        pages = page_table.shape[1]
        group = HK // (kvl * head_dim)
        heads = kvl * group
        T = ffn_seat.shape[0]
        R, DK = resid.shape
        FK = w_gate.shape[1]
        WC = divisor(DK, (WCM, 512, 256, 128))
        NJ = DK // WC
        CF = divisor(FK, (256, 128))
        NC = FK // CF
        half = T // 2
        NX = nc // 2
        KB, FB = DK // TILE, FK // TILE
        dims = (
            T, B, R, HK, DK, FK, kvl, group, pages, blocks, WC, NJ, CF, NC, half, NX, float(DK * nd)
        )
        dma = pltpu.SemaphoreType.DMA
        hbm = pl.BlockSpec(memory_space=pltpu.HBM)
        vmem = pltpu.VMEM
        PB = B // 2
        scratch = [
            pltpu.SMEM((pages, B), jnp.int32),
            pltpu.SMEM((B,), jnp.int32),
            vmem((B, HK), BF16),
            vmem((1, T), jnp.int32),
            vmem((T, DK), BF16),
            vmem((T, DK), BF16),
            vmem((T, T), BF16),
            vmem((1, DK), F32),
            vmem((HK, DK), BF16),
            vmem((DK, FK), BF16),
            vmem((DK, FK), BF16),
            vmem((max(blocks * kvl, (KB + 1) // 2 * FB), TILE, TILE), BF16),
            vmem((max(blocks * kvl, (KB + 1) // 2 * FB), TILE, TILE), BF16),
            vmem((B * heads, head_dim), F32),
            vmem((PB * heads, head_dim), F32),
            vmem((B * heads, pages * page), F32),
            vmem((T, HK), BF16),
            vmem((T, DK), BF16),
            vmem((2, half // 2, DK), BF16),
            vmem((2, half // 2, DK), BF16),
            vmem((2, max(NX - 1, 1), half // 2, DK), BF16),
            vmem((T, DK), BF16),
            vmem((2, half // 2, DK), F32),
            vmem((NC, 2, half, 2 * CF), BF16),
            vmem((NC, half, 2 * CF), BF16),
            vmem((NC, half, 2 * CF), BF16),
            vmem((T, 128), F32),
            vmem((half, 128), F32),
            vmem((half, 128), F32),
            vmem((half, 128), F32),
            vmem((NC, T, CF), BF16),
            vmem((T, DK), F32),
            vmem((NX * R, DK), BF16),
            vmem((NX * R, DK), BF16),
            vmem((max(NX - 1, 1), R, DK), BF16),
            dma((6,)),
            dma((2,)),
            dma((5,)),
            dma((2, nd, 2)),
            dma((nd, 2)),
            dma((2, 2)),
            dma((nc - 1,)),
            dma((nc - 1,)),
            dma((2,)),
            dma((2, NJ)),
            dma((2, max(NX - 1, 1))),
            dma((2, max(NX - 1, 1), NJ)),
            dma((2,)),
            dma((2,)),
            dma((2,)),
            dma((2, NC, PART)),
            dma((2,)),
            dma((2,)),
            dma((2,)),
            dma((2, NC, PART)),
            dma((1,)),
            dma((NJ,)),
            dma((max(NX - 1, 1),)),
            dma((max(NX - 1, 1), NJ)),
        ]
        return pl.pallas_call(
            functools.partial(layer_kernel, nd, nc, dims),
            out_shape=pltpu.VMEM((R, DK), BF16),
            in_specs=[hbm] * 11,
            out_specs=pl.BlockSpec(memory_space=pltpu.VMEM),
            scratch_shapes=scratch,
            compiler_params=pltpu.CompilerParams(
                collective_id=0, has_side_effects=True, vmem_limit_bytes=67043328 - 2 * R * DK
            ),
        )(
            page_table.T,
            seq_lengths,
            queries,
            kv_pages.reshape(blocks * kvl, 2, page, head_dim),
            ffn_seat[None, :],
            resid,
            norm_gain[None, :],
            w_out,
            w_gate,
            w_up,
            w_down.reshape(FB, TILE, DK),
        )

    in_specs = (
        P(("rep", "dev"), "col"),
        P(("rep", "dev"), "col", None, None, None),
        P(("rep", "dev"), None),
        P(("rep", "dev")),
        P("rep"),
        P(("rep", "col"), "dev"),
        P("col", "dev"),
        P("dev"),
        P("dev", "col"),
        P("dev", "col"),
        P("col", "dev"),
    )
    return jax.shard_map(
        on_device,
        mesh=mesh,
        in_specs=in_specs,
        out_specs=P(("rep", "col"), "dev"),
        check_vma=False,
    )
```

```python
import functools

import jax
import jax.numpy as jnp
from jax import lax
from jax.experimental import pallas as pl
from jax.experimental.pallas import tpu as pltpu
from jax.sharding import PartitionSpec as P

MESH = pl.DeviceIdType.MESH
F32 = jnp.float32
BF16 = jnp.bfloat16
TILE = 128
SUB = 8
LATER = 5
END_PROJ = 2
END_GAP = 2
PART = 1
WCM = 1024
LAG_S0 = 4
LAG_S = 3
LAG_H0 = 3
LAG_H = 4


def divisor(size, choices):
    for choice in choices:
        if size % choice == 0:
            return choice
    return size


def layer_kernel(
    nd,
    nc,
    dims,
    table_hbm,
    len_hbm,
    q_hbm,
    kv_hbm,
    seat_hbm,
    resid_hbm,
    gain_hbm,
    wo_hbm,
    wg_hbm,
    wu_hbm,
    wd_hbm,
    out,
    table,
    lens,
    q_in,
    seat,
    resid_all,
    resid_rows,
    pick,
    gain,
    wo,
    wg,
    wu,
    kpool,
    vpool,
    q_rows,
    o_rows,
    scores,
    att_all,
    proj,
    rs_one,
    rs_mid,
    rs_two,
    x_all,
    stream,
    own,
    in_r,
    in_l,
    ss_own,
    ss_r,
    ss_l,
    inv,
    hid,
    acc,
    dn_one,
    dn_mid,
    dn_two,
    in_sem,
    kv_sem,
    w_sem,
    att_s,
    att_r,
    far_s,
    res_s,
    res_r,
    one_s,
    one_r,
    two_s,
    two_r,
    pair_s,
    pair_r,
    sum_s,
    sum_r,
    ssd_s,
    ssd_r,
    hid_s,
    hid_r,
    done_s,
    done_r,
    dtwo_s,
    dtwo_r,
):
    T, B, R, HK, DK, FK, kvl, group, pages, blocks, WC, NJ, CF, NC, half, NX, full = dims
    RH = half // nc
    PACE = 2 if NC % 2 == 0 else 1
    PHASE = NC // PACE
    MID_START = max(PHASE, LATER + 2)
    END_START = MID_START + END_GAP
    me = lax.axis_index("dev")
    mc = lax.axis_index("col")
    mx, core = mc // 2, mc % 2
    E = nd - 1
    late_dev = (me * 2) // nd
    halves = (late_dev, 1 - late_dev)
    heads = kvl * group
    span = pages * TILE
    KB = DK // TILE
    FB = FK // TILE
    KH = (KB + 1) // 2
    partner = {"col": mx * 2 + 1 - core}

    def peer_of(k):
        return lax.rem(mc + k, nc)

    def x_peer(k):
        return lax.rem(mx + k, NX)

    def x_from(k):
        return lax.rem(mx + NX - k, NX)

    small = [
        pltpu.make_async_copy(table_hbm, table, in_sem.at[0]),
        pltpu.make_async_copy(len_hbm, lens, in_sem.at[1]),
        pltpu.make_async_copy(q_hbm, q_in, in_sem.at[2]),
        pltpu.make_async_copy(seat_hbm, seat, in_sem.at[3]),
        pltpu.make_async_copy(
            resid_hbm, resid_all.at[pl.ds(pl.multiple_of(mc * R, R), R), :], in_sem.at[4]
        ),
        pltpu.make_async_copy(gain_hbm, gain, in_sem.at[5]),
    ]
    kv_count = blocks * kvl
    kv_copies = [
        pltpu.make_async_copy(
            kv_hbm.at[:, v], (kpool, vpool)[v].at[pl.ds(0, kv_count)], kv_sem.at[v]
        )
        for v in (0, 1)
    ]
    w_copies = [
        pltpu.make_async_copy(wo_hbm, wo, w_sem.at[0]),
        pltpu.make_async_copy(wg_hbm, wg, w_sem.at[1]),
        pltpu.make_async_copy(wu_hbm, wu, w_sem.at[2]),
    ]

    def wd_copy(n):
        cols = slice(n * TILE, (n + 1) * TILE)
        return pltpu.make_async_copy(
            wd_hbm.at[:, :, cols],
            (kpool, vpool)[n // KH].at[pl.ds(n % KH * FB, FB)],
            w_sem.at[3 + n // KH],
        )

    def wd_wait():
        for n, target in enumerate((kpool, vpool)):
            count = min(KH, KB - n * KH)
            if count > 0:
                spot = target.at[pl.ds(0, count * FB)]
                pltpu.make_async_copy(spot, spot, w_sem.at[3 + n]).wait()

    for copy in small:
        copy.start()
    for copy in kv_copies:
        copy.start()

    barrier = pltpu.get_barrier_semaphore()

    @pl.when(me > 0)
    def _():
        pl.semaphore_signal(barrier, inc=1, device_id={"dev": me - 1}, device_id_type=MESH)

    @pl.when(me < E)
    def _():
        pl.semaphore_signal(barrier, inc=1, device_id={"dev": me + 1}, device_id_type=MESH)

    for here, there in ((E - 2, E), (E, E - 2), (2, 0), (0, 2)):
        @pl.when(me == here)
        def _():
            pl.semaphore_signal(barrier, inc=1, device_id={"dev": there}, device_id_type=MESH)

    for k in range(1, nc):
        pl.semaphore_signal(barrier, inc=1, device_id={"col": peer_of(k)}, device_id_type=MESH)

    small[2].wait()
    for n in range(heads):
        q_rows[pl.ds(n, B, stride=heads), :] = q_in[:, n * TILE : (n + 1) * TILE].astype(F32)
    small[0].wait()
    small[1].wait()
    def res_copy(k):
        spot = resid_all.at[pl.ds(pl.multiple_of(mc * R, R), R), :]
        return pltpu.make_async_remote_copy(
            src_ref=spot,
            dst_ref=spot,
            send_sem=res_s.at[k - 1],
            recv_sem=res_r.at[k - 1],
            device_id={"col": peer_of(k)},
            device_id_type=MESH,
        )

    neighbours = jnp.where(me > 0, 1, 0) + jnp.where(me < E, 1, 0)
    for here in (E - 2, E, 2, 0):
        neighbours = neighbours + jnp.where(me == here, 1, 0)
    for copy in small[3:]:
        copy.wait()
    pl.semaphore_wait(barrier, neighbours + nc - 1)
    for k in range(1, nc):
        res_copy(k).start()
    kv_copies[0].wait()
    w_copies[0].start()

    PB = B // 2
    scale = TILE ** (-0.5)
    head_row = lax.broadcasted_iota(jnp.int32, (heads, TILE), 0) // group

    def blocked(value):
        if kvl == 1:
            return value.astype(BF16)
        wide = lax.broadcasted_iota(jnp.int32, value.shape, 0) // group
        return jnp.concatenate(
            [jnp.where(wide == h, value, 0.0).astype(BF16) for h in range(kvl)], axis=1
        )

    def att_copy(origin, a, way):
        spot = att_all.at[pl.ds(pl.multiple_of(origin * B + a * PB, PB), PB), :]
        return pltpu.make_async_remote_copy(
            src_ref=spot,
            dst_ref=spot,
            send_sem=att_s.at[way, origin, a],
            recv_sem=att_r.at[origin, a],
            device_id={"dev": me + (1 if way == 0 else -1)},
            device_id_type=MESH,
        )

    if True:
        @pl.loop(0, B // SUB)
        def _(b):
            for u in range(SUB):
                s = spot = b * SUB + u
                rows = pl.ds(pl.multiple_of(s * heads, heads), heads)
                query = blocked(q_rows[rows, :])
                keys = []
                for j in range(pages):
                    block = table[j, s]
                    keys.append(
                        jnp.concatenate([kpool[block * kvl + h] for h in range(kvl)], axis=1)
                        if kvl > 1
                        else kpool[block]
                    )
                value = lax.dot_general(
                    query,
                    jnp.concatenate(keys, axis=0),
                    (((1,), (1,)), ((), ())),
                    preferred_element_type=F32,
                ) * scale
                live = lax.broadcasted_iota(jnp.int32, value.shape, 1) < lens[s]
                scores[pl.ds(pl.multiple_of(spot * heads, heads), heads), :] = jnp.where(
                    live, value, -1e30
                )

    kv_copies[1].wait()
    w_copies[1].start()
    w_copies[2].start()
    def far_copy(way, a):
        origin = 0 if way == 0 else E
        spot = att_all.at[pl.ds(origin * B + a * PB, PB), :]
        return pltpu.make_async_remote_copy(
            src_ref=spot,
            dst_ref=spot,
            send_sem=far_s.at[way, a],
            recv_sem=att_r.at[origin, a],
            device_id={"dev": E - origin},
            device_id_type=MESH,
        )

    for a in range(2):

        @pl.loop(0, PB // SUB)
        def _(b):
            base = a * PB + b * SUB
            rows = pl.ds(pl.multiple_of(base * heads, SUB * heads), SUB * heads)
            value = scores[rows, :]
            expo = jnp.exp(value - jnp.max(value, axis=1, keepdims=True))
            scores[rows, :] = expo / jnp.sum(expo, axis=1, keepdims=True)
            for u in range(SUB):
                spot = b * SUB + u
                s = a * PB + spot
                weights = blocked(scores[pl.ds(pl.multiple_of(s * heads, heads), heads), :])
                vals = [
                    vpool[table[j, s] * kvl + h]
                    for h in range(kvl)
                    for j in range(pages)
                ]
                o_rows[pl.ds(pl.multiple_of(spot * heads, heads), heads), :] = jnp.dot(
                    weights, jnp.concatenate(vals, axis=0), preferred_element_type=F32
                )

        mine = pl.ds(pl.multiple_of(me * B + a * PB, PB), PB)
        for n in range(heads):
            att_all[mine, n * TILE : (n + 1) * TILE] = o_rows[
                pl.ds(n, PB, stride=heads), :
            ].astype(BF16)

        @pl.when(me < E)
        def _():
            att_copy(me, a, 0).start()

        @pl.when(me > 0)
        def _():
            att_copy(me, a, 1).start()

    for n in range(KB):
        wd_copy(n).start()

    place = lax.broadcasted_iota(jnp.int32, (T, T), 0)
    position = place // R
    seat_here = ((position % NX) * 2 + position // NX) * R + place % R
    pick[...] = (seat_here == seat[...]).astype(F32).astype(BF16)
    fetch = (place == seat[...]).astype(F32).astype(BF16)

    def passes(origin, way):
        if way == 0:
            return jnp.logical_and(me < E, jnp.logical_or(origin > 0, me + 1 < E))
        return jnp.logical_and(me > 0, jnp.logical_or(origin < E, me - 1 > 0))

    def take(origin, way, relay):
        inside = origin >= 0 if way == 0 else origin <= E
        move = passes(origin, way)
        wanted = move if relay else jnp.logical_not(move)

        @pl.when(jnp.logical_and(inside, wanted))
        def _():
            for a in range(2):
                att_copy(origin, a, way).wait_recv()
                if relay:
                    att_copy(origin, a, way).start()

                    @pl.when(
                        jnp.logical_and(
                            me == (E - 2 if way == 0 else 2), origin == (0 if way == 0 else E)
                        )
                    )
                    def _():
                        far_copy(way, a).start()

    def both(k, relay):
        take(me - k, 0, relay)
        take(me + k, 1, relay)

    @pl.loop(1, nd // 2)
    def _(k):
        both(k, True)
        both(k, False)

    half_rows = NX * RH

    def rows_of(step, c, x, count=1):
        start = halves[step] * half + (c * NX + x) * RH
        return pl.ds(pl.multiple_of(start, RH), count * RH)

    mid_own = pl.ds(pl.multiple_of(mx * RH, RH), RH)

    def whole(spot, send, recv):
        return pltpu.make_async_remote_copy(
            src_ref=spot,
            dst_ref=spot,
            send_sem=send,
            recv_sem=recv,
            device_id=partner,
            device_id_type=MESH,
        )

    def one_copy(step, j):
        cols = slice(j * WC, (j + 1) * WC)
        return pltpu.make_async_remote_copy(
            src_ref=proj.at[rows_of(step, 1 - core, 0, NX), cols],
            dst_ref=rs_one.at[step, :, cols],
            send_sem=one_s.at[step],
            recv_sem=one_r.at[step, j],
            device_id=partner,
            device_id_type=MESH,
        )

    def two_copy(step, k, j):
        cols = slice(j * WC, (j + 1) * WC)
        return pltpu.make_async_remote_copy(
            src_ref=rs_mid.at[step, :, cols],
            dst_ref=rs_two.at[step, k - 1, :, cols],
            send_sem=two_s.at[step, k - 1],
            recv_sem=two_r.at[step, k - 1, j],
            device_id={"col": x_peer(k) * 2 + core},
            device_id_type=MESH,
        )

    def project(step, j):
        cols = slice(j * WC, (j + 1) * WC)
        rows = pl.ds(pl.multiple_of(halves[step] * half, half), half)
        proj[rows, cols] = jnp.dot(
            att_all[rows, :], wo[:, cols], preferred_element_type=F32
        ).astype(BF16)
        one_copy(step, j).start()

    def meet(step, j):
        cols = slice(j * WC, (j + 1) * WC)
        one_copy(step, j).wait_recv()
        rs_mid[step, :, cols] = (
            proj[rows_of(step, core, 0, NX), cols].astype(F32) + rs_one[step, :, cols].astype(F32)
        ).astype(BF16)
        for k in range(1, NX):
            two_copy(step, k, j).start()

    def pair_copy(step, j):
        spot = x_all.at[rows_of(step, core, 0, NX), j * WC : (j + 1) * WC]
        return pltpu.make_async_remote_copy(
            src_ref=spot,
            dst_ref=spot,
            send_sem=pair_s.at[step],
            recv_sem=pair_r.at[step],
            device_id=partner,
            device_id_type=MESH,
        )

    def streams(step):
        rows = rows_of(step, core, 0, NX)
        for j in range(NJ):
            cols = slice(j * WC, (j + 1) * WC)
            value = (
                resid_rows[rows, cols].astype(F32)
                + proj[rows, cols].astype(F32)
                + rs_one[step, :, cols].astype(F32)
            )
            for k in range(1, NX):
                two_copy(step, k, j).wait_recv()
                value = value + rs_two[step, k - 1, :, cols].astype(F32)
            stream[step, :, cols] = value
            x_all[rows, cols] = (value * gain[:, cols]).astype(BF16)
            pair_copy(step, j).start()

    def x_arrive(step):
        spot = x_all.at[rows_of(step, 1 - core, 0, NX), :]
        whole(spot, pair_s.at[step], pair_r.at[step]).wait_recv()

    w_copies[0].wait()
    for j in range(NJ + 1):
        if j < NJ:
            project(0, j)
        if j > 0:
            meet(0, j - 1)

    @pl.loop(nd // 2, nd)
    def _(k):
        both(k, True)

    for k in range(1, nc):
        res_copy(k).wait_recv()
    for j in range(NJ):
        cols = slice(j * WC, (j + 1) * WC)
        resid_rows[:, cols] = lax.dot_general(
            fetch, resid_all[:, cols], (((0,), (0,)), ((), ())), preferred_element_type=F32
        ).astype(BF16)

    is_end = jnp.logical_or(me == 0, me == E)

    def second_part():
        @pl.loop(nd // 2, nd)
        def _(k):
            both(k, False)

        for j in range(NJ):
            project(1, j)

    @pl.when(jnp.logical_not(is_end))
    def _():
        second_part()

    streams(0)

    @pl.when(jnp.logical_not(is_end))
    def _():
        for j in range(NJ):
            meet(1, j)

    x_arrive(0)
    def neighbour(way):
        return {"dev": me + (1 if way == 0 else -1)}

    RQ = half // PART

    def sum_copy(way, c, r):
        rows = slice(r * RQ, (r + 1) * RQ)
        return pltpu.make_async_remote_copy(
            src_ref=own.at[c, way, rows, :],
            dst_ref=(in_r if way == 0 else in_l).at[c, rows, :],
            send_sem=sum_s.at[way],
            recv_sem=sum_r.at[way, c, r],
            device_id=neighbour(way),
            device_id_type=MESH,
        )

    def ssd_copy(way):
        return pltpu.make_async_remote_copy(
            src_ref=ss_own.at[pl.ds(way * half, half), :],
            dst_ref=ss_r if way == 0 else ss_l,
            send_sem=ssd_s.at[way],
            recv_sem=ssd_r.at[way],
            device_id=neighbour(way),
            device_id_type=MESH,
        )

    def hid_copy(way, c, r):
        spot = hid.at[c, pl.ds((1 - way) * half + r * RQ, RQ), :]
        return pltpu.make_async_remote_copy(
            src_ref=spot,
            dst_ref=spot,
            send_sem=hid_s.at[way],
            recv_sem=hid_r.at[way, c, r],
            device_id=neighbour(way),
            device_id_type=MESH,
        )

    def sum_stage(way, c):
        first = 0 if way == 0 else E
        last = E - first
        part = way
        incoming = in_r if way == 0 else in_l
        ss_in = ss_r if way == 0 else ss_l
        ss_rows = pl.ds(part * half, half)

        @pl.when(c == jnp.where(me == last, 0, min(1, NC - 1)))
        def _():
            ssd_copy(way).wait_recv()
            ss_own[ss_rows, :] = ss_own[ss_rows, :] + ss_in[...]

            @pl.when(me != last)
            def _():
                ssd_copy(way).start()

            @pl.when(me == last)
            def _():
                inv[...] = lax.rsqrt(ss_own[ss_rows, :] / full + 1e-5)

        for r in range(PART):
            rows = slice(r * RQ, (r + 1) * RQ)
            sum_copy(way, c, r).wait_recv()
            total = own[c, part, rows, :].astype(F32) + incoming[c, rows, :].astype(F32)

            @pl.when(me != last)
            def _():
                own[c, part, rows, :] = total.astype(BF16)
                sum_copy(way, c, r).start()

            @pl.when(me == last)
            def _():
                factor = inv[rows, 0:1]
                gate = total[:, :CF] * factor
                up = total[:, CF:] * factor
                hid[c, part * half + r * RQ : part * half + (r + 1) * RQ, :] = (
                    gate / (1.0 + jnp.exp(-gate)) * up
                ).astype(BF16)
                hid_copy(1 - way, c, r).start()

    def hid_stage(way, c):
        last = E if way == 0 else 0
        for r in range(PART):
            hid_copy(way, c, r).wait_recv()

            @pl.when(me != last)
            def _():
                hid_copy(way, c, r).start()

    def inside(c):
        return jnp.logical_and(c >= 0, c < NC)

    def sum_lag(d):
        return LAG_S0 + LAG_S * (d - 1)

    first_hid = max(NC + LAG_H0, sum_lag(E) + 1)

    def hid_lag(d):
        return first_hid + LAG_H * (d - 1)

    acc[...] = jnp.zeros_like(acc)
    w_copies[1].wait()
    w_copies[2].wait()

    second_start = jnp.where(is_end, END_START, MID_START)

    @pl.loop(0, NC + hid_lag(E))
    def _(i):
        again = i >= second_start
        turn = jnp.where(again, halves[1], halves[0])
        turn_rows = pl.ds(pl.multiple_of(turn * half, half), half)
        place_in = jnp.where(again, i - second_start, i)

        @pl.when(jnp.logical_and(is_end, i == END_PROJ))
        def _():
            second_part()

        @pl.when(jnp.logical_and(is_end, i == END_PROJ + 2))
        def _():
            for j in range(NJ):
                meet(1, j)

        @pl.when(i == jnp.where(is_end, END_START - 1, LATER))
        def _():
            streams(1)

        @pl.when(i == second_start)
        def _():
            x_arrive(1)
        @pl.when(place_in < PHASE)
        def _():
            value = x_all[turn_rows, :]
            for p in range(PACE):
                q = place_in * PACE + p
                cols = pl.ds(pl.multiple_of(q * CF, CF), CF)
                own[q, turn, :, :CF] = jnp.dot(
                    value, wg[:, cols], preferred_element_type=F32
                ).astype(BF16)
                own[q, turn, :, CF:] = jnp.dot(
                    value, wu[:, cols], preferred_element_type=F32
                ).astype(BF16)

        for way in (0, 1):
            @pl.when(jnp.logical_and(i < PHASE, me == (0 if way == 0 else E)))
            def _():
                for p in range(PACE):
                    for r in range(PART):
                        sum_copy(way, i * PACE + p, r).start()

        @pl.when(place_in == 0)
        def _():
            squares = jnp.zeros((half, 1), F32)
            for j in range(NJ):
                cols = slice(j * WC, (j + 1) * WC)
                value = x_all[turn_rows, cols].astype(F32) / gain[:, cols]
                squares = squares + jnp.sum(value * value, axis=1, keepdims=True)
            ss_own[turn_rows, :] = jnp.broadcast_to(squares, (half, ss_own.shape[1]))
            for way in (0, 1):
                @pl.when(jnp.logical_and(i == 0, me == (0 if way == 0 else E)))
                def _():
                    ssd_copy(way).start()

        for way in (0, 1):
            d = me if way == 0 else E - me
            c = i - sum_lag(d)

            @pl.when(jnp.logical_and(d > 0, inside(c)))
            def _():
                sum_stage(way, c)

        for way in (0, 1):
            d = me if way == 0 else E - me
            c = i - hid_lag(d)

            @pl.when(jnp.logical_and(d > 0, inside(c)))
            def _():
                hid_stage(way, c)

        c = i - hid_lag(jnp.maximum(me, E - me))

        @pl.when(i == hid_lag(jnp.maximum(me, E - me)))
        def _():
            wd_wait()

        @pl.when(inside(c))
        def _():
            per = CF // TILE
            wide = 2 if KB % 2 == 0 else 1
            value = hid[c]
            for n in range(0, KB, wide):
                right = [
                    (kpool, vpool)[(n + w) // KH][
                        pl.ds((n + w) % KH * FB + c * per, per)
                    ].reshape(CF, TILE)
                    for w in range(wide)
                ]
                cols = slice(n * TILE, (n + wide) * TILE)
                acc[:, cols] += jnp.dot(
                    value, jnp.concatenate(right, axis=1), preferred_element_type=F32
                )

    down = resid_rows
    my_half = pl.ds(pl.multiple_of(core * NX * R, R), NX * R)
    other_half = pl.ds(pl.multiple_of((1 - core) * NX * R, R), NX * R)

    def done_copy(j):
        cols = slice(j * WC, (j + 1) * WC)
        return pltpu.make_async_remote_copy(
            src_ref=down.at[other_half, cols],
            dst_ref=dn_one.at[:, cols],
            send_sem=done_s.at[0],
            recv_sem=done_r.at[j],
            device_id=partner,
            device_id_type=MESH,
        )

    def last_copy(k, j):
        cols = slice(j * WC, (j + 1) * WC)
        rows = pl.ds(pl.multiple_of(x_peer(k) * R, R), R)
        return pltpu.make_async_remote_copy(
            src_ref=dn_mid.at[rows, cols],
            dst_ref=dn_two.at[k - 1, :, cols],
            send_sem=dtwo_s.at[k - 1],
            recv_sem=dtwo_r.at[k - 1, j],
            device_id={"col": x_peer(k) * 2 + core},
            device_id_type=MESH,
        )

    for step in (0, 1):
        rows = rows_of(step, core, mx)
        acc[rows, :] = acc[rows, :] + stream[step, mid_own, :]
    for j in range(NJ + 1):
        if j < NJ:
            cols = slice(j * WC, (j + 1) * WC)
            down[:, cols] = jnp.dot(
                pick[...], acc[:, cols].astype(BF16), preferred_element_type=F32
            ).astype(BF16)
            done_copy(j).start()
        if j > 0:
            cols = slice((j - 1) * WC, j * WC)
            done_copy(j - 1).wait_recv()
            dn_mid[:, cols] = (
                down[my_half, cols].astype(F32) + dn_one[:, cols].astype(F32)
            ).astype(BF16)
            for k in range(1, NX):
                last_copy(k, j - 1).start()
    my_rows = pl.ds(pl.multiple_of((core * NX + mx) * R, R), R)
    my_mid = pl.ds(pl.multiple_of(mx * R, R), R)
    for j in range(NJ):
        cols = slice(j * WC, (j + 1) * WC)
        value = down[my_rows, cols].astype(F32) + dn_one[my_mid, cols].astype(F32)
        for k in range(1, NX):
            last_copy(k, j).wait_recv()
            value = value + dn_two[k - 1, :, cols].astype(F32)
        out[:, cols] = value.astype(BF16)

    for k in range(1, nc):
        res_copy(k).wait_send()
    for step in (0, 1):
        mine = x_all.at[rows_of(step, core, 0, NX), :]
        whole(proj.at[rows_of(step, 1 - core, 0, NX), :], one_s.at[step], one_r.at[step, 0]).wait_send()
        for k in range(1, NX):
            whole(mine, two_s.at[step, k - 1], one_r.at[step, 0]).wait_send()
        whole(mine, pair_s.at[step], one_r.at[step, 0]).wait_send()
    whole(down.at[other_half, :], done_s.at[0], done_r.at[0]).wait_send()
    for k in range(1, NX):
        whole(down.at[my_rows, :], dtwo_s.at[k - 1], done_r.at[0]).wait_send()

    for way in (0, 1):
        @pl.when(me == (E - 2 if way == 0 else 2))
        def _():
            for a in range(2):
                far_copy(way, a).wait_send()

    for a in range(2):
        @pl.loop(0, nd)
        def _(origin):
            left = jnp.logical_or(origin == me, jnp.logical_and(origin < me, passes(origin, 0)))
            right = jnp.logical_or(origin == me, jnp.logical_and(origin > me, passes(origin, 1)))

            @pl.when(jnp.logical_and(me < E, left))
            def _():
                att_copy(origin, a, 0).wait_send()

            @pl.when(jnp.logical_and(me > 0, right))
            def _():
                att_copy(origin, a, 1).wait_send()

    for way in (0, 1):
        @pl.when(me != (E if way == 0 else 0))
        def _():
            ssd_copy(way).wait_send()

            whole(own.at[:, way], sum_s.at[way], sum_r.at[way, 0, 0]).wait_send()
            sent = hid.at[:, pl.ds((1 - way) * half, half), :]
            whole(sent, hid_s.at[way], hid_r.at[way, 0, 0]).wait_send()


def solution(mesh):
    nd, nc = mesh.shape["dev"], mesh.shape["col"]

    def on_device(
        queries,
        kv_pages,
        page_table,
        seq_lengths,
        ffn_seat,
        resid,
        w_out,
        norm_gain,
        w_gate,
        w_up,
        w_down,
    ):
        B, HK = queries.shape
        blocks, kvl, _, page, head_dim = kv_pages.shape
        pages = page_table.shape[1]
        group = HK // (kvl * head_dim)
        heads = kvl * group
        T = ffn_seat.shape[0]
        R, DK = resid.shape
        FK = w_gate.shape[1]
        WC = divisor(DK, (WCM, 512, 256, 128))
        NJ = DK // WC
        CF = divisor(FK, (256, 128))
        NC = FK // CF
        half = T // 2
        NX = nc // 2
        KB, FB = DK // TILE, FK // TILE
        dims = (
            T, B, R, HK, DK, FK, kvl, group, pages, blocks, WC, NJ, CF, NC, half, NX, float(DK * nd)
        )
        dma = pltpu.SemaphoreType.DMA
        hbm = pl.BlockSpec(memory_space=pltpu.HBM)
        vmem = pltpu.VMEM
        PB = B // 2
        scratch = [
            pltpu.SMEM((pages, B), jnp.int32),
            pltpu.SMEM((B,), jnp.int32),
            vmem((B, HK), BF16),
            vmem((1, T), jnp.int32),
            vmem((T, DK), BF16),
            vmem((T, DK), BF16),
            vmem((T, T), BF16),
            vmem((1, DK), F32),
            vmem((HK, DK), BF16),
            vmem((DK, FK), BF16),
            vmem((DK, FK), BF16),
            vmem((max(blocks * kvl, (KB + 1) // 2 * FB), TILE, TILE), BF16),
            vmem((max(blocks * kvl, (KB + 1) // 2 * FB), TILE, TILE), BF16),
            vmem((B * heads, head_dim), F32),
            vmem((PB * heads, head_dim), F32),
            vmem((B * heads, pages * page), F32),
            vmem((T, HK), BF16),
            vmem((T, DK), BF16),
            vmem((2, half // 2, DK), BF16),
            vmem((2, half // 2, DK), BF16),
            vmem((2, max(NX - 1, 1), half // 2, DK), BF16),
            vmem((T, DK), BF16),
            vmem((2, half // 2, DK), F32),
            vmem((NC, 2, half, 2 * CF), BF16),
            vmem((NC, half, 2 * CF), BF16),
            vmem((NC, half, 2 * CF), BF16),
            vmem((T, 128), F32),
            vmem((half, 128), F32),
            vmem((half, 128), F32),
            vmem((half, 128), F32),
            vmem((NC, T, CF), BF16),
            vmem((T, DK), F32),
            vmem((NX * R, DK), BF16),
            vmem((NX * R, DK), BF16),
            vmem((max(NX - 1, 1), R, DK), BF16),
            dma((6,)),
            dma((2,)),
            dma((5,)),
            dma((2, nd, 2)),
            dma((nd, 2)),
            dma((2, 2)),
            dma((nc - 1,)),
            dma((nc - 1,)),
            dma((2,)),
            dma((2, NJ)),
            dma((2, max(NX - 1, 1))),
            dma((2, max(NX - 1, 1), NJ)),
            dma((2,)),
            dma((2,)),
            dma((2,)),
            dma((2, NC, PART)),
            dma((2,)),
            dma((2,)),
            dma((2,)),
            dma((2, NC, PART)),
            dma((1,)),
            dma((NJ,)),
            dma((max(NX - 1, 1),)),
            dma((max(NX - 1, 1), NJ)),
        ]
        return pl.pallas_call(
            functools.partial(layer_kernel, nd, nc, dims),
            out_shape=pltpu.VMEM((R, DK), BF16),
            in_specs=[hbm] * 11,
            out_specs=pl.BlockSpec(memory_space=pltpu.VMEM),
            scratch_shapes=scratch,
            compiler_params=pltpu.CompilerParams(
                collective_id=0, has_side_effects=True, vmem_limit_bytes=67043328 - 2 * R * DK
            ),
        )(
            page_table.T,
            seq_lengths,
            queries,
            kv_pages.reshape(blocks * kvl, 2, page, head_dim),
            ffn_seat[None, :],
            resid,
            norm_gain[None, :],
            w_out,
            w_gate,
            w_up,
            w_down.reshape(FB, TILE, DK),
        )

    in_specs = (
        P(("rep", "dev"), "col"),
        P(("rep", "dev"), "col", None, None, None),
        P(("rep", "dev"), None),
        P(("rep", "dev")),
        P("rep"),
        P(("rep", "col"), "dev"),
        P("col", "dev"),
        P("dev"),
        P("dev", "col"),
        P("dev", "col"),
        P("col", "dev"),
    )
    return jax.shard_map(
        on_device,
        mesh=mesh,
        in_specs=in_specs,
        out_specs=P(("rep", "col"), "dev"),
        check_vma=False,
    )
```
